256 devices in a mesh: xy: 64 (over z_hi, y, x, core), gz: 4 (over z_lo).
Axes of the slice: x: 4, y: 4, z: 8 (z_hi: 2, z_lo: 4; z = z_hi * 4 + z_lo), core: 2. Of those that a mesh axis runs over, the one named last changes fastest.
Arguments:
- field: float32 [64, 2, 3, 512, 256], P('gz', None, None, 'xy'), may hold values from -6 to 6
- source: float32 [64, 2, 3, 512, 256], P('gz', None, None, 'xy'), may hold values from -6 to 6
- classes: int32 [64, 512, 256], P('gz', 'xy'), may hold values from 0 to 15
- boundary: int32 [64, 512, 256], P('gz', 'xy'), may hold values 0 or 1
- conductance: float32 [16], replicated, may hold values from 0.001 to 1
- angles: float32 [3], replicated, may hold values from -3.140625 to 3.140625
- strengths: float32 [3], replicated, may hold values from 0.5 to 2
Outputs:
- relaxed: float32 [64, 2, 3, 512, 256], P('gz', None, None, 'xy')
The draws below stay inside these ranges and needn't reach their ends.
All inputs are finite; a program needn't handle non-finite values. No bound on the sum of `boundary` on one device may be relied on, other than what follows from the above.
Results may differ from the reference program's by a relative error of at most 0.00029.
Values sent between devices are 32-bit elements; how exact they have to be, the bound alone decides.
A program may use at most 64 MiB of HBM per device.

```python
import math
import jax
import jax.numpy as jnp
from jax import lax

NX = 256
CLASSES = 16
SWEEPS = 2
NZ = 64
NY = 512


def touch_ends(array, stream_key, least, largest):
    extent = array.shape
    place = [jax.random.randint(jax.random.fold_in(stream_key, axis), (), 0, extent[axis]) for axis in range(len(extent))]
    array = array.at[tuple(place)].set(least)
    longest = extent.index(max(extent))
    place[longest] = (place[longest] + 1) % extent[longest]
    return array.at[tuple(place)].set(largest)


def block_levels(rng, dims, pieces, least, largest):
    def one(position, blocks):
        steps = jax.random.uniform(jax.random.fold_in(jax.random.fold_in(rng, 6), position), (blocks,), jnp.float32, least / len(pieces), largest / len(pieces))
        return jnp.repeat(jnp.exp(steps), dims[position] // blocks).reshape((-1,) + (1,) * (len(dims) - position - 1))

    loudness = one(*pieces[0])
    for cut in pieces[1:]:
        loudness = loudness * one(*cut)
    return loudness


def scatter_about(key, extent, width, limit, split=(), kind=jnp.bfloat16):
    gain = block_levels(key, extent, split, -0.22, 0.18) if split else 1.0
    values = jax.random.normal(key, extent, jnp.float32) * width * gain
    return jnp.minimum(jnp.maximum(values, -limit), limit).astype(kind)


def setup_inputs(seed: int = 0) -> dict:
    keys = jax.random.split(jax.random.key(seed), 8)
    return {
        "field": scatter_about(keys[0], (NZ, 2, 3, NY, NX), 1.0, 6.0, ((0, 4), (3, 64)), jnp.float32),
        "source": scatter_about(keys[1], (NZ, 2, 3, NY, NX), 1.0, 6.0, ((0, 4), (3, 64)), jnp.float32),
        "classes": touch_ends(jax.random.randint(keys[2], (NZ, NY, NX), 0, CLASSES), jax.random.fold_in(keys[2], 1), 0, CLASSES - 1).astype(jnp.int32),
        "boundary": touch_ends((jax.random.randint(keys[3], (NZ, NY, NX), 0, 8) < 1).astype(jnp.int32), jax.random.fold_in(keys[3], 1), 0, 1),
        "conductance": jnp.clip(jnp.exp(jax.random.uniform(keys[4], (CLASSES,), jnp.float32, math.log(0.001), math.log(1.0))), 0.001, 1.0),
        "angles": jnp.clip(jax.random.uniform(keys[5], (3,), jnp.float32, -3.140625, 3.140625), -3.140625, 3.140625),
        "strengths": jnp.clip(jnp.exp(jax.random.uniform(keys[6], (3,), jnp.float32, math.log(0.5), math.log(2.0))), 0.5, 2.0),
    }


coupling = 0.1
penalty = 4.0


def about_depth(cosine, sine_val):
    filler = jnp.zeros_like(cosine)
    ones_fill = jnp.ones_like(cosine)
    return jnp.stack([jnp.stack([cosine, -sine_val, filler]), jnp.stack([sine_val, cosine, filler]), jnp.stack([filler, filler, ones_fill])])


def about_north(cosine, sine_val):
    filler = jnp.zeros_like(cosine)
    ones_fill = jnp.ones_like(cosine)
    return jnp.stack([jnp.stack([cosine, filler, sine_val]), jnp.stack([filler, ones_fill, filler]), jnp.stack([-sine_val, filler, cosine])])


def rotation(angles):
    cosines = jnp.cos(angles)
    sines = jnp.sin(angles)
    first = jnp.dot(about_depth(cosines[0], sines[0]), about_north(cosines[1], sines[1]), precision=lax.Precision.HIGHEST)
    return jnp.dot(first, about_depth(cosines[2], sines[2]), precision=lax.Precision.HIGHEST)


def sweep_forward(driven, diag_real, diag_imag, start):
    def advance(previous, slices):
        inverse, earlier = previous
        forcing, diag_re, diag_im = slices
        pivot_re = diag_re[None] - inverse[0]
        pivot_im = diag_im - inverse[1]
        weight_sq = 1.0 / (pivot_re * pivot_re + pivot_im * pivot_im)
        new_inverse = jnp.stack([pivot_re * weight_sq, -pivot_im * weight_sq])
        new_earlier = jnp.stack([forcing[0] + inverse[0] * earlier[0] - inverse[1] * earlier[1],
                                 forcing[1] + inverse[0] * earlier[1] + inverse[1] * earlier[0]])
        return (new_inverse, new_earlier), (new_inverse, new_earlier)

    last_state, history = lax.scan(advance, start, (driven, diag_real, diag_imag))
    return history


def sweep_backward(inverse_all, carried_all, start):
    def advance(following, slices):
        inverse, carried = slices
        summed = carried + following
        result = jnp.stack([inverse[0] * summed[0] - inverse[1] * summed[1],
                            inverse[0] * summed[1] + inverse[1] * summed[0]])
        return result, result

    last_state, history = lax.scan(advance, start, (inverse_all, carried_all), reverse=True)
    return history


def reference(field, source, classes, boundary, conductance, angles, strengths):
    rotation_matrix = rotation(angles)
    diag_real = 2.0 + 4.0 * coupling + penalty * boundary.astype(jnp.float32)
    diag_imag = conductance[classes][:, None] * strengths[None, :, None, None]
    current = field
    for repeat in range(SWEEPS):
        padded = jnp.pad(current, ((0, 0), (0, 0), (0, 0), (1, 1), (1, 1)))
        beside = padded[:, :, :, 2:, 1:-1] + padded[:, :, :, :-2, 1:-1] + padded[:, :, :, 1:-1, 2:] + padded[:, :, :, 1:-1, :-2]
        driven = source + coupling * beside
        turned = jnp.einsum('cj,zpcyx->zpjyx', rotation_matrix, driven, precision=lax.Precision.HIGHEST)
        blank = jnp.zeros(turned.shape[1:], jnp.float32)
        inverse_all, carried_all = sweep_forward(turned, diag_real, diag_imag, (blank, blank))
        solved = sweep_backward(inverse_all, carried_all, blank)
        current = jnp.einsum('cj,zpjyx->zpcyx', rotation_matrix, solved, precision=lax.Precision.HIGHEST)
    return current
```

```python
import functools

import jax
import jax.numpy as jnp
from jax import lax
from jax.experimental import pallas as pl
from jax.experimental.pallas import tpu as pltpu
from jax.sharding import PartitionSpec as P

SWEEPS = 2
COUPLING = 0.1
PENALTY = 4.0
CHUNKS = 4
MESH = pl.DeviceIdType.MESH


def mul(left, right):
    return (left[0] * right[0] - left[1] * right[1], left[0] * right[1] + left[1] * right[0])


def add(left, right):
    return (left[0] + right[0], left[1] + right[1])


def inverse(value):
    weight = 1.0 / (value[0] * value[0] + value[1] * value[1])
    return (value[0] * weight, -(value[1] * weight))


def one_less(value):
    return (1.0 - value[0], -value[1])


def get(ref, *index):
    return (ref[(*index, 0)], ref[(*index, 1)])


def put(ref, value, *index):
    ref[(*index, 0)] = value[0]
    ref[(*index, 1)] = value[1]


def look_up(table_ref, count, index):
    values = [table_ref[c] for c in range(count)]
    bit = 1
    while len(values) > 1:
        odd = (index & bit) != 0
        values = [
            jnp.where(odd, values[n + 1], values[n]) if n + 1 < len(values) else values[n]
            for n in range(0, len(values), 2)
        ]
        bit *= 2
    return values[0]


def rotation(angles_ref):
    turns = [jnp.full((8, 128), angles_ref[n], jnp.float32) for n in range(3)]
    c0, c1, c2 = [jnp.cos(t)[0, 0] for t in turns]
    s0, s1, s2 = [jnp.sin(t)[0, 0] for t in turns]
    first = [[c0 * c1, -s0, c0 * s1], [s0 * c1, c0, s0 * s1], [-s1, jnp.float32(0.0), c1]]
    return [[f[0] * c2 + f[1] * s2, f[1] * c2 - f[0] * s2, f[2]] for f in first]


def kernel(
    ni, nk,
    field, source, classes, boundary, conductance, angles, strengths,
    out,
    cur, src, cls, bnd, piv, vec_v, vec_u, sol,
    ends, coef_r, coef_c,
    halo_out, halo_in, chain_out, chain_in,
    load_sem, halo_send, halo_recv, chain_send, chain_recv,
):
    i = lax.axis_index("xy")
    k = lax.axis_index("gz")
    depth, _, comps, rows, lanes = cur.shape
    per = depth // CHUNKS
    last = depth - 1

    loads = [
        pltpu.make_async_copy(a, b, load_sem.at[n])
        for n, (a, b) in enumerate(((field, cur), (classes, cls), (boundary, bnd), (source, src)))
    ]
    for copy in loads:
        copy.start()

    barrier = pltpu.get_barrier_semaphore()
    neighbours = (
        (i > 0, {"xy": i - 1}),
        (i < ni - 1, {"xy": i + 1}),
        (k > 0, {"gz": k - 1}),
        (k < nk - 1, {"gz": k + 1}),
    )
    for there, target in neighbours:
        @pl.when(there)
        def _():
            pl.semaphore_signal(barrier, inc=1, device_id=target, device_id_type=MESH)

    @pl.when(i == 0)
    def _():
        for n in range(SWEEPS):
            halo_in[n, 0] = jnp.zeros(halo_in.shape[2:], jnp.float32)

    @pl.when(i == ni - 1)
    def _():
        for n in range(SWEEPS):
            halo_in[n, 1] = jnp.zeros(halo_in.shape[2:], jnp.float32)

    @pl.when(k == 0)
    def _():
        for n in range(SWEEPS + 1):
            chain_in[n, 0] = jnp.zeros(chain_in.shape[2:], jnp.float32)

    @pl.when(k == nk - 1)
    def _():
        for n in range(SWEEPS + 1):
            chain_in[n, 1] = jnp.zeros(chain_in.shape[2:], jnp.float32)

    turn = rotation(angles)

    def halo_copy(number, side, chunk):
        part = pl.ds(chunk * per, per)
        return pltpu.make_async_remote_copy(
            src_ref=halo_out.at[number, side, part],
            dst_ref=halo_in.at[number, 1 - side, part],
            send_sem=halo_send.at[number, side, chunk],
            recv_sem=halo_recv.at[number, 1 - side, chunk],
            device_id={"xy": i + 2 * side - 1},
            device_id_type=MESH,
        )

    sides = ((0, i > 0), (1, i < ni - 1))

    def send_halo(number, chunk):
        for side, there in sides:
            @pl.when(there)
            def _():
                halo_copy(number, side, chunk).start()

    def wait_halo(number):
        for side, there in sides:
            @pl.when(there)
            def _():
                for chunk in range(CHUNKS):
                    halo_copy(number, 1 - side, chunk).wait_recv()

    def finish_halo(number):
        for side, there in sides:
            @pl.when(there)
            def _():
                for chunk in range(CHUNKS):
                    halo_copy(number, side, chunk).wait_send()

    def chain_copy(stage, way, comp):
        return pltpu.make_async_remote_copy(
            src_ref=chain_out.at[stage, way, comp],
            dst_ref=chain_in.at[stage, way, comp],
            send_sem=chain_send.at[stage, way, comp],
            recv_sem=chain_recv.at[stage, way, comp],
            device_id={"gz": k + 1 - 2 * way},
            device_id_type=MESH,
        )

    def run_chain(stage, step):
        near_half = lax.div(k * 2, nk)
        for order in range(2):
            way = near_half if order == 0 else 1 - near_half
            has_in = jnp.where(way == 0, k, nk - 1 - k) > 0
            has_out = jnp.where(way == 0, nk - 1 - k, k) > 0
            for comp in range(comps):
                @pl.when(has_in)
                def _():
                    chain_copy(stage, way, comp).wait_recv()

                put(chain_out, step(way, comp, get(chain_in, stage, way, comp)), stage, way, comp)

                @pl.when(has_out)
                def _():
                    chain_copy(stage, way, comp).start()

    def finish_chain(stage):
        for way, there in ((0, k < nk - 1), (1, k > 0)):
            @pl.when(there)
            def _():
                for comp in range(comps):
                    chain_copy(stage, way, comp).wait_send()

    pl.semaphore_wait(barrier, sum(there.astype(jnp.int32) for there, _ in neighbours))

    loads[0].wait()
    for chunk in range(CHUNKS):
        for z in range(chunk * per, (chunk + 1) * per):
            for part in range(2):
                here = cur[z, part]
                halo_out[0, 0, z, part] = here[:, :1]
                halo_out[0, 1, z, part] = here[:, rows - 1:]
        send_halo(0, chunk)

    loads[1].wait()
    loads[2].wait()
    for z in range(depth):
        sigma = look_up(conductance, conductance.shape[0], cls[z])
        real = (2.0 + 4.0 * COUPLING) + PENALTY * bnd[z].astype(jnp.float32)
        for comp in range(comps):
            diagonal = (real, sigma * strengths[comp])
            if z:
                before = get(piv, z - 1, comp)
                diagonal = (diagonal[0] - before[0], diagonal[1] - before[1])
            pivot = inverse(diagonal)
            put(piv, pivot, z, comp)
            if z == 1:
                put(vec_v, before, z, comp)
            elif z > 1:
                put(vec_v, mul(before, get(vec_v, z - 1, comp)), z, comp)
    for comp in range(comps):
        pivot = get(piv, last, comp)
        column_v, column_u = mul(pivot, get(vec_v, last, comp)), pivot
        put(vec_v, column_v, last, comp)
        put(vec_u, column_u, last, comp)
        put(ends, column_u, 1, comp)
        for z in range(last - 1, -1, -1):
            pivot = get(piv, z, comp)
            column_u = mul(pivot, column_u)
            put(vec_u, column_u, z, comp)
            if z:
                column_v = mul(pivot, add(get(vec_v, z, comp), column_v))
            else:
                column_v = mul(pivot, (1.0 + column_v[0], column_v[1]))
            put(vec_v, column_v, z, comp)
        put(ends, column_v, 0, comp)

    def coefficient_step(way, comp, arrived):
        near, far = get(ends, way, comp), get(ends, 1 - way, comp)
        across = get(vec_u, 0, comp)
        passed = mul(across, inverse(one_less(mul(near, arrived))))
        put(coef_c, passed, way, comp)
        linked = mul(passed, arrived)
        put(coef_r, linked, way, comp)
        return add(far, mul(linked, across))

    run_chain(0, coefficient_step)

    loads[3].wait()
    sublane = lax.broadcasted_iota(jnp.int32, (comps, rows, lanes), 1)
    lane = lax.broadcasted_iota(jnp.int32, (comps, rows, lanes), 2)

    for number in range(SWEEPS):
        stage = number + 1
        wait_halo(number)
        carried = None
        for z in range(depth):
            turned = []
            for part in range(2):
                here = cur[z, part]
                up = jnp.where(sublane == 0, halo_in[number, 0, z, part], pltpu.roll(here, 1, 1))
                down = jnp.where(
                    sublane == rows - 1, halo_in[number, 1, z, part], pltpu.roll(here, rows - 1, 1)
                )
                left = jnp.where(lane == 0, 0.0, pltpu.roll(here, 1, 2))
                right = jnp.where(lane == lanes - 1, 0.0, pltpu.roll(here, lanes - 1, 2))
                driven = src[z, part] + COUPLING * ((down + up) + (right + left))
                turned.append([
                    turn[0][j] * driven[0] + turn[1][j] * driven[1] + turn[2][j] * driven[2]
                    for j in range(comps)
                ])
            for comp in range(comps):
                forcing = (turned[0][comp], turned[1][comp])
                if z:
                    forcing = add(forcing, mul(get(piv, z - 1, comp), get(sol, z - 1, comp)))
                put(sol, forcing, z, comp)
        for comp in range(comps):
            value = mul(get(piv, last, comp), get(sol, last, comp))
            put(sol, value, last, comp)
            for z in range(last - 1, -1, -1):
                value = mul(get(piv, z, comp), add(get(sol, z, comp), value))
                put(sol, value, z, comp)

        def forcing_step(way, comp, arrived):
            near = get(sol, last * way, comp)
            far = get(sol, last * (1 - way), comp)
            local = add(far, mul(get(coef_r, way, comp), near))
            return add(local, mul(get(coef_c, way, comp), arrived))

        run_chain(stage, forcing_step)

        first_in, last_in = [], []
        for comp in range(comps):
            p_in, q_in = get(chain_in, 0, 0, comp), get(chain_in, 0, 1, comp)
            p_out, q_out = get(chain_out, 0, 0, comp), get(chain_out, 0, 1, comp)
            above = add(get(chain_in, stage, 0, comp), mul(p_in, get(chain_out, stage, 1, comp)))
            below = add(get(chain_in, stage, 1, comp), mul(q_in, get(chain_out, stage, 0, comp)))
            first_in.append(mul(above, inverse(one_less(mul(q_out, p_in)))))
            last_in.append(mul(below, inverse(one_less(mul(p_out, q_in)))))
        for chunk in range(CHUNKS):
            for z in range(chunk * per, (chunk + 1) * per):
                solved = []
                for comp in range(comps):
                    value = add(
                        mul(get(vec_v, z, comp), first_in[comp]),
                        mul(get(vec_u, z, comp), last_in[comp]),
                    )
                    solved.append(add(get(sol, z, comp), value))
                for part in range(2):
                    for c in range(comps):
                        value = (
                            turn[c][0] * solved[0][part]
                            + turn[c][1] * solved[1][part]
                            + turn[c][2] * solved[2][part]
                        )
                        if stage == SWEEPS:
                            out[z, part, c] = value
                        else:
                            cur[z, part, c] = value
                            halo_out[stage, 0, z, part, c] = value[:1]
                            halo_out[stage, 1, z, part, c] = value[rows - 1:]
            if stage < SWEEPS:
                send_halo(stage, chunk)

    for number in range(SWEEPS):
        finish_halo(number)
    for stage in range(SWEEPS + 1):
        finish_chain(stage)


def local(ni, nk, field, source, classes, boundary, conductance, angles, strengths):
    depth, _, comps, rows, lanes = field.shape
    block = (depth, 2, comps, rows, lanes)
    lines = (depth, comps, 2, rows, lanes)
    ends = (2, comps, 2, rows, lanes)
    vmem = lambda *shape: pltpu.VMEM(shape, jnp.float32)
    dma = lambda *shape: pltpu.SemaphoreType.DMA(shape)
    whole = pl.BlockSpec(memory_space=pltpu.HBM)
    scalars = pl.BlockSpec(memory_space=pltpu.SMEM)
    return pl.pallas_call(
        functools.partial(kernel, ni, nk),
        out_shape=jax.ShapeDtypeStruct(block, jnp.float32),
        in_specs=[whole] * 4 + [scalars] * 3,
        out_specs=pl.BlockSpec(memory_space=pltpu.VMEM),
        scratch_shapes=[
            vmem(*block), vmem(*block),
            pltpu.VMEM(classes.shape, jnp.int32), pltpu.VMEM(boundary.shape, jnp.int32),
            vmem(*lines), vmem(*lines), vmem(*lines), vmem(*lines),
            vmem(*ends), vmem(*ends), vmem(*ends),
            vmem(SWEEPS, 2, depth, 2, comps, 1, lanes), vmem(SWEEPS, 2, depth, 2, comps, 1, lanes),
            vmem(SWEEPS + 1, *ends), vmem(SWEEPS + 1, *ends),
            dma(4), dma(SWEEPS, 2, CHUNKS), dma(SWEEPS, 2, CHUNKS),
            dma(SWEEPS + 1, 2, comps), dma(SWEEPS + 1, 2, comps),
        ],
        compiler_params=pltpu.CompilerParams(
            collective_id=0, has_side_effects=True, vmem_limit_bytes=67043328
        ),
    )(field, source, classes, boundary, conductance, angles, strengths)


def solution(mesh):
    in_specs = (
        P("gz", None, None, "xy", None),
        P("gz", None, None, "xy", None),
        P("gz", "xy", None),
        P("gz", "xy", None),
        P(),
        P(),
        P(),
    )
    out_specs = P("gz", None, None, "xy", None)
    body = functools.partial(local, mesh.shape["xy"], mesh.shape["gz"])
    return jax.shard_map(body, mesh=mesh, in_specs=in_specs, out_specs=out_specs, check_vma=False)
```

```python
import functools

import jax
import jax.numpy as jnp
from jax import lax
from jax.experimental import pallas as pl
from jax.experimental.pallas import tpu as pltpu
from jax.sharding import PartitionSpec as P

SWEEPS = 2
COUPLING = 0.1
PENALTY = 4.0
CHUNKS = 4
MESH = pl.DeviceIdType.MESH


def mul(left, right):
    return (left[0] * right[0] - left[1] * right[1], left[0] * right[1] + left[1] * right[0])


def add(left, right):
    return (left[0] + right[0], left[1] + right[1])


def inverse(value):
    weight = 1.0 / (value[0] * value[0] + value[1] * value[1])
    return (value[0] * weight, -(value[1] * weight))


def one_less(value):
    return (1.0 - value[0], -value[1])


def get(ref, *index):
    return (ref[(*index, 0)], ref[(*index, 1)])


def put(ref, value, *index):
    ref[(*index, 0)] = value[0]
    ref[(*index, 1)] = value[1]


def look_up(table_ref, count, index):
    values = [table_ref[c] for c in range(count)]
    bit = 1
    while len(values) > 1:
        odd = (index & bit) != 0
        values = [
            jnp.where(odd, values[n + 1], values[n]) if n + 1 < len(values) else values[n]
            for n in range(0, len(values), 2)
        ]
        bit *= 2
    return values[0]


def rotation(angles_ref):
    turns = [jnp.full((8, 128), angles_ref[n], jnp.float32) for n in range(3)]
    c0, c1, c2 = [jnp.cos(t)[0, 0] for t in turns]
    s0, s1, s2 = [jnp.sin(t)[0, 0] for t in turns]
    first = [[c0 * c1, -s0, c0 * s1], [s0 * c1, c0, s0 * s1], [-s1, jnp.float32(0.0), c1]]
    return [[f[0] * c2 + f[1] * s2, f[1] * c2 - f[0] * s2, f[2]] for f in first]


def kernel(
    ni, nk,
    field, source, classes, boundary, conductance, angles, strengths,
    out,
    cur, src, cls, bnd, piv, vec_v, vec_u, rhs, sol,
    ends, coef_r, coef_c,
    halo_out, halo_in, chain_out, chain_in, edge_out, edge_in,
    load_sem, halo_send, halo_recv, chain_send, chain_recv, edge_send, edge_recv,
):
    i = lax.axis_index("xy")
    k = lax.axis_index("gz")
    depth, _, comps, rows, lanes = cur.shape
    per = depth // CHUNKS
    last = depth - 1

    loads = [
        pltpu.make_async_copy(a, b, load_sem.at[n])
        for n, (a, b) in enumerate(((field, cur), (classes, cls), (boundary, bnd), (source, src)))
    ]
    for copy in loads:
        copy.start()

    barrier = pltpu.get_barrier_semaphore()
    neighbours = [(i > 0, {"xy": i - 1}), (i < ni - 1, {"xy": i + 1})]
    for far in range(1, nk):
        neighbours += [(k >= far, {"gz": k - far}), (k < nk - far, {"gz": k + far})]
    for there, target in neighbours:
        @pl.when(there)
        def _():
            pl.semaphore_signal(barrier, inc=1, device_id=target, device_id_type=MESH)

    for side, alone in ((0, i == 0), (1, i == ni - 1)):
        @pl.when(alone)
        def _():
            for n in range(SWEEPS):
                halo_in[n, side] = jnp.zeros(halo_in.shape[2:], jnp.float32)

    for way, place in ((0, k), (1, nk - 1 - k)):
        @pl.when(place == 0)
        def _():
            for n in range(SWEEPS + 1):
                chain_in[n, way] = jnp.zeros(chain_in.shape[2:], jnp.float32)

        for far in range(1, nk):
            @pl.when(place < far)
            def _():
                for n in range(SWEEPS + 1):
                    edge_in[n, way, far - 1] = jnp.zeros(edge_in.shape[3:], jnp.float32)

    turn = rotation(angles)

    def halo_copy(number, side, chunk):
        part = pl.ds(chunk * per, per)
        return pltpu.make_async_remote_copy(
            src_ref=halo_out.at[number, side, part],
            dst_ref=halo_in.at[number, 1 - side, part],
            send_sem=halo_send.at[number, side, chunk],
            recv_sem=halo_recv.at[number, 1 - side, chunk],
            device_id={"xy": i + 2 * side - 1},
            device_id_type=MESH,
        )

    sides = ((0, i > 0), (1, i < ni - 1))

    def send_halo(number, chunk):
        for side, there in sides:
            @pl.when(there)
            def _():
                halo_copy(number, side, chunk).start()

    def wait_halo(number):
        for side, there in sides:
            @pl.when(there)
            def _():
                for chunk in range(CHUNKS):
                    halo_copy(number, 1 - side, chunk).wait_recv()

    def finish_halo(number):
        for side, there in sides:
            @pl.when(there)
            def _():
                for chunk in range(CHUNKS):
                    halo_copy(number, side, chunk).wait_send()

    def place_of(way):
        return jnp.where(way == 0, k, nk - 1 - k)

    def chain_copy(stage, way, comp):
        return pltpu.make_async_remote_copy(
            src_ref=chain_out.at[stage, way, comp],
            dst_ref=chain_in.at[stage, way, comp],
            send_sem=chain_send.at[stage, way, comp],
            recv_sem=chain_recv.at[stage, way, comp],
            device_id={"gz": k + 1 - 2 * way},
            device_id_type=MESH,
        )

    def relay(stage, way, step):
        for comp in range(comps):
            @pl.when(place_of(way) > 0)
            def _():
                chain_copy(stage, way, comp).wait_recv()

            put(chain_out, step(way, comp, get(chain_in, stage, way, comp)), stage, way, comp)

            @pl.when(place_of(way) < nk - 1)
            def _():
                chain_copy(stage, way, comp).start()

    def finish_chain(stage):
        for way, there in ((0, k < nk - 1), (1, k > 0)):
            @pl.when(there)
            def _():
                for comp in range(comps):
                    chain_copy(stage, way, comp).wait_send()

    def edge_copy(stage, way, far):
        return pltpu.make_async_remote_copy(
            src_ref=edge_out.at[stage, way],
            dst_ref=edge_in.at[stage, way, far - 1],
            send_sem=edge_send.at[stage, way, far - 1],
            recv_sem=edge_recv.at[stage, way, far - 1],
            device_id={"gz": k + far * (1 - 2 * way)},
            device_id_type=MESH,
        )

    def send_edges(stage, way, values):
        for comp in range(comps):
            for part in range(2):
                edge_out[stage, way, comp, part, :1] = values[comp][part][:1]
                edge_out[stage, way, comp, part, 1:] = values[comp][part][rows - 1:]
        for far in range(nk - 1, 0, -1):
            @pl.when(place_of(way) < nk - far)
            def _():
                edge_copy(stage, way, far).start()

    def wait_edges(stage):
        for way in range(2):
            for far in range(1, nk):
                @pl.when(place_of(way) >= far)
                def _():
                    edge_copy(stage, way, far).wait_recv()

    def finish_edges(stage):
        for way in range(2):
            for far in range(1, nk):
                @pl.when(place_of(way) < nk - far)
                def _():
                    edge_copy(stage, way, far).wait_send()

    loads[0].wait()
    for z in range(depth):
        for part in range(2):
            here = cur[z, part]
            halo_out[0, 0, z, part] = here[:, :1]
            halo_out[0, 1, z, part] = here[:, rows - 1:]

    loads[1].wait()
    loads[2].wait()
    for z in range(depth):
        sigma = look_up(conductance, conductance.shape[0], cls[z])
        real = (2.0 + 4.0 * COUPLING) + PENALTY * bnd[z].astype(jnp.float32)
        for comp in range(comps):
            diagonal = (real, sigma * strengths[comp])
            if z:
                before = get(piv, z - 1, comp)
                diagonal = (diagonal[0] - before[0], diagonal[1] - before[1])
            pivot = inverse(diagonal)
            put(piv, pivot, z, comp)
            if z == 1:
                put(vec_v, before, z, comp)
            elif z > 1:
                put(vec_v, mul(before, get(vec_v, z - 1, comp)), z, comp)
    for comp in range(comps):
        pivot = get(piv, last, comp)
        column_v, column_u = mul(pivot, get(vec_v, last, comp)), pivot
        put(vec_v, column_v, last, comp)
        put(vec_u, column_u, last, comp)
        put(ends, column_u, 1, comp)
        for z in range(last - 1, -1, -1):
            pivot = get(piv, z, comp)
            column_u = mul(pivot, column_u)
            put(vec_u, column_u, z, comp)
            if z:
                column_v = mul(pivot, add(get(vec_v, z, comp), column_v))
            else:
                column_v = mul(pivot, (1.0 + column_v[0], column_v[1]))
            put(vec_v, column_v, z, comp)
        put(ends, column_v, 0, comp)

    pl.semaphore_wait(barrier, sum(there.astype(jnp.int32) for there, _ in neighbours))
    for chunk in range(CHUNKS):
        send_halo(0, chunk)

    def coefficient_step(way, comp, arrived):
        near, far = get(ends, way, comp), get(ends, 1 - way, comp)
        across = get(vec_u, 0, comp)
        passed = mul(across, inverse(one_less(mul(near, arrived))))
        put(coef_c, passed, way, comp)
        linked = mul(passed, arrived)
        put(coef_r, linked, way, comp)
        return add(far, mul(linked, across))

    def relay_coefficients(way):
        relay(0, way, coefficient_step)
        send_edges(0, way, [get(coef_c, way, comp) for comp in range(comps)])

    def local_forcing(way, comp):
        near = get(sol, last * way, comp)
        far = get(sol, last * (1 - way), comp)
        return add(far, mul(get(coef_r, way, comp), near))

    def forcing_step(way, comp, arrived):
        return add(local_forcing(way, comp), mul(get(coef_c, way, comp), arrived))

    def send_forcing_edges(stage, way):
        send_edges(stage, way, [local_forcing(way, comp) for comp in range(comps)])

    sublane = lax.broadcasted_iota(jnp.int32, (comps, rows, lanes), 1)
    lane = lax.broadcasted_iota(jnp.int32, (comps, rows, lanes), 2)
    plane = lax.broadcasted_iota(jnp.int32, (rows, lanes), 0)

    def turned_back(vectors):
        return [
            turn[0][j] * vectors[0] + turn[1][j] * vectors[1] + turn[2][j] * vectors[2]
            for j in range(comps)
        ]

    def without_halo():
        for z in range(depth):
            for part in range(2):
                here = cur[z, part]
                up = jnp.where(sublane == 0, 0.0, pltpu.roll(here, 1, 1))
                down = jnp.where(sublane == rows - 1, 0.0, pltpu.roll(here, rows - 1, 1))
                left = jnp.where(lane == 0, 0.0, pltpu.roll(here, 1, 2))
                right = jnp.where(lane == lanes - 1, 0.0, pltpu.roll(here, lanes - 1, 2))
                driven = src[z, part] + COUPLING * ((down + up) + (right + left))
                for comp, value in enumerate(turned_back(driven)):
                    rhs[z, comp, part] = value
            forward(z, [get(rhs, z, comp) for comp in range(comps)])
        backward()

    def with_halo(number):
        for z in range(depth):
            added = []
            for part in range(2):
                outer = jnp.where(
                    sublane == 0,
                    halo_in[number, 0, z, part],
                    jnp.where(sublane == rows - 1, halo_in[number, 1, z, part], 0.0),
                )
                added.append(turned_back(COUPLING * outer))
            forward(z, [
                add(get(rhs, z, comp), (added[0][comp], added[1][comp])) for comp in range(comps)
            ])
        backward()

    def forward(z, forcings):
        for comp, forcing in enumerate(forcings):
            if z:
                forcing = add(forcing, mul(get(piv, z - 1, comp), get(sol, z - 1, comp)))
            put(sol, forcing, z, comp)

    def backward():
        for comp in range(comps):
            value = mul(get(piv, last, comp), get(sol, last, comp))
            put(sol, value, last, comp)
            for z in range(last - 1, -1, -1):
                value = mul(get(piv, z, comp), add(get(sol, z, comp), value))
                put(sol, value, z, comp)

    near_way = lax.div(k * 2, nk)
    far_way = 1 - near_way

    @pl.when(place_of(near_way) == 0)
    def _():
        relay_coefficients(near_way)

    loads[3].wait()
    for number in range(SWEEPS):
        stage = number + 1
        without_halo()
        if number == 0:
            @pl.when(place_of(near_way) > 0)
            def _():
                relay_coefficients(near_way)

        relay(stage, near_way, forcing_step)
        wait_halo(number)
        with_halo(number)
        send_forcing_edges(stage, near_way)
        if number == 0:
            relay_coefficients(far_way)
        send_forcing_edges(stage, far_way)
        relay(stage, far_way, forcing_step)

        if number == 0:
            wait_edges(0)
        wait_edges(stage)
        first_in, last_in = [], []
        for comp in range(comps):
            arrived, leaving = [], []
            for way in range(2):
                total = None
                for far in range(nk - 1, 0, -1):
                    term = get(edge_in, stage, way, far - 1, comp)
                    if total is not None:
                        term = add(term, mul(get(edge_in, 0, way, far - 1, comp), total))
                    total = term
                inner = get(chain_in, stage, way, comp)
                value = tuple(
                    jnp.where(
                        plane == 0,
                        total[part][:1],
                        jnp.where(plane == rows - 1, total[part][1:], inner[part]),
                    )
                    for part in range(2)
                )
                arrived.append(value)
                leaving.append(forcing_step(way, comp, value))
            p_in, q_in = get(chain_in, 0, 0, comp), get(chain_in, 0, 1, comp)
            p_out, q_out = get(chain_out, 0, 0, comp), get(chain_out, 0, 1, comp)
            above = add(arrived[0], mul(p_in, leaving[1]))
            below = add(arrived[1], mul(q_in, leaving[0]))
            first_in.append(mul(above, inverse(one_less(mul(q_out, p_in)))))
            last_in.append(mul(below, inverse(one_less(mul(p_out, q_in)))))
        for chunk in range(CHUNKS):
            for z in range(chunk * per, (chunk + 1) * per):
                solved = []
                for comp in range(comps):
                    value = add(
                        mul(get(vec_v, z, comp), first_in[comp]),
                        mul(get(vec_u, z, comp), last_in[comp]),
                    )
                    solved.append(add(get(sol, z, comp), value))
                for part in range(2):
                    for c in range(comps):
                        value = (
                            turn[c][0] * solved[0][part]
                            + turn[c][1] * solved[1][part]
                            + turn[c][2] * solved[2][part]
                        )
                        if stage == SWEEPS:
                            out[z, part, c] = value
                        else:
                            cur[z, part, c] = value
                            halo_out[stage, 0, z, part, c] = value[:1]
                            halo_out[stage, 1, z, part, c] = value[rows - 1:]
            if stage < SWEEPS:
                send_halo(stage, chunk)

    for number in range(SWEEPS):
        finish_halo(number)
    for stage in range(SWEEPS + 1):
        finish_chain(stage)
        finish_edges(stage)


def local(ni, nk, field, source, classes, boundary, conductance, angles, strengths):
    depth, _, comps, rows, lanes = field.shape
    block = (depth, 2, comps, rows, lanes)
    lines = (depth, comps, 2, rows, lanes)
    ends = (2, comps, 2, rows, lanes)
    vmem = lambda *shape: pltpu.VMEM(shape, jnp.float32)
    dma = lambda *shape: pltpu.SemaphoreType.DMA(shape)
    whole = pl.BlockSpec(memory_space=pltpu.HBM)
    scalars = pl.BlockSpec(memory_space=pltpu.SMEM)
    return pl.pallas_call(
        functools.partial(kernel, ni, nk),
        out_shape=jax.ShapeDtypeStruct(block, jnp.float32),
        in_specs=[whole] * 4 + [scalars] * 3,
        out_specs=pl.BlockSpec(memory_space=pltpu.VMEM),
        scratch_shapes=[
            vmem(*block), vmem(*block),
            pltpu.VMEM(classes.shape, jnp.int32), pltpu.VMEM(boundary.shape, jnp.int32),
            vmem(*lines), vmem(*lines), vmem(*lines), vmem(*lines), vmem(*lines),
            vmem(*ends), vmem(*ends), vmem(*ends),
            vmem(SWEEPS, 2, depth, 2, comps, 1, lanes), vmem(SWEEPS, 2, depth, 2, comps, 1, lanes),
            vmem(SWEEPS + 1, *ends), vmem(SWEEPS + 1, *ends),
            vmem(SWEEPS + 1, 2, comps, 2, 2, lanes), vmem(SWEEPS + 1, 2, nk - 1, comps, 2, 2, lanes),
            dma(4), dma(SWEEPS, 2, CHUNKS), dma(SWEEPS, 2, CHUNKS),
            dma(SWEEPS + 1, 2, comps), dma(SWEEPS + 1, 2, comps),
            dma(SWEEPS + 1, 2, nk - 1), dma(SWEEPS + 1, 2, nk - 1),
        ],
        compiler_params=pltpu.CompilerParams(
            collective_id=0, has_side_effects=True, vmem_limit_bytes=67043328
        ),
    )(field, source, classes, boundary, conductance, angles, strengths)


def solution(mesh):
    in_specs = (
        P("gz", None, None, "xy", None),
        P("gz", None, None, "xy", None),
        P("gz", "xy", None),
        P("gz", "xy", None),
        P(),
        P(),
        P(),
    )
    out_specs = P("gz", None, None, "xy", None)
    body = functools.partial(local, mesh.shape["xy"], mesh.shape["gz"])
    return jax.shard_map(body, mesh=mesh, in_specs=in_specs, out_specs=out_specs, check_vma=False)
```

```python
import functools

import jax
import jax.numpy as jnp
from jax import lax
from jax.experimental import pallas as pl
from jax.experimental.pallas import tpu as pltpu
from jax.sharding import PartitionSpec as P

SWEEPS = 2
COUPLING = 0.1
PENALTY = 4.0
CHUNKS = 4
MESH = pl.DeviceIdType.MESH


def mul(left, right):
    return (left[0] * right[0] - left[1] * right[1], left[0] * right[1] + left[1] * right[0])


def add(left, right):
    return (left[0] + right[0], left[1] + right[1])


def inverse(value):
    weight = 1.0 / (value[0] * value[0] + value[1] * value[1])
    return (value[0] * weight, -(value[1] * weight))


def one_less(value):
    return (1.0 - value[0], -value[1])


def get(ref, *index):
    return (ref[(*index, 0)], ref[(*index, 1)])


def put(ref, value, *index):
    ref[(*index, 0)] = value[0]
    ref[(*index, 1)] = value[1]


def look_up(table_ref, count, index):
    values = [table_ref[c] for c in range(count)]
    bit = 1
    while len(values) > 1:
        odd = (index & bit) != 0
        values = [
            jnp.where(odd, values[n + 1], values[n]) if n + 1 < len(values) else values[n]
            for n in range(0, len(values), 2)
        ]
        bit *= 2
    return values[0]


def rotation(angles_ref):
    turns = [jnp.full((8, 128), angles_ref[n], jnp.float32) for n in range(3)]
    c0, c1, c2 = [jnp.cos(t)[0, 0] for t in turns]
    s0, s1, s2 = [jnp.sin(t)[0, 0] for t in turns]
    first = [[c0 * c1, -s0, c0 * s1], [s0 * c1, c0, s0 * s1], [-s1, jnp.float32(0.0), c1]]
    return [[f[0] * c2 + f[1] * s2, f[1] * c2 - f[0] * s2, f[2]] for f in first]


def kernel(
    ni, nk,
    field, source, classes, boundary, conductance, angles, strengths,
    out,
    cur, src, cls, bnd, piv, vec_v, vec_u, rhs, sol,
    ends, coef_r, coef_c,
    halo_out, halo_in, chain_out, chain_in, edge_out, edge_in,
    load_sem, halo_send, halo_recv, chain_send, chain_recv, edge_send, edge_recv,
):
    i = lax.axis_index("xy")
    k = lax.axis_index("gz")
    depth, _, comps, rows, lanes = cur.shape
    per = depth // CHUNKS
    last = depth - 1

    loads = [
        pltpu.make_async_copy(a, b, load_sem.at[n])
        for n, (a, b) in enumerate(((field, cur), (classes, cls), (boundary, bnd), (source, src)))
    ]
    for copy in loads:
        copy.start()

    barrier = pltpu.get_barrier_semaphore()
    neighbours = [(i > 0, {"xy": i - 1}), (i < ni - 1, {"xy": i + 1})]
    for far in range(1, nk):
        neighbours += [(k >= far, {"gz": k - far}), (k < nk - far, {"gz": k + far})]
    for there, target in neighbours:
        @pl.when(there)
        def _():
            pl.semaphore_signal(barrier, inc=1, device_id=target, device_id_type=MESH)

    for side, alone in ((0, i == 0), (1, i == ni - 1)):
        @pl.when(alone)
        def _():
            for n in range(SWEEPS):
                halo_in[n, side] = jnp.zeros(halo_in.shape[2:], jnp.float32)

    for way, place in ((0, k), (1, nk - 1 - k)):
        @pl.when(place == 0)
        def _():
            for n in range(SWEEPS + 1):
                chain_in[n, way] = jnp.zeros(chain_in.shape[2:], jnp.float32)

        for far in range(1, nk):
            @pl.when(place < far)
            def _():
                for n in range(SWEEPS + 1):
                    edge_in[n, way, far - 1] = jnp.zeros(edge_in.shape[3:], jnp.float32)

    turn = rotation(angles)

    def halo_copy(number, side, chunk):
        part = pl.ds(chunk * per, per)
        return pltpu.make_async_remote_copy(
            src_ref=halo_out.at[number, side, part],
            dst_ref=halo_in.at[number, 1 - side, part],
            send_sem=halo_send.at[number, side, chunk],
            recv_sem=halo_recv.at[number, 1 - side, chunk],
            device_id={"xy": i + 2 * side - 1},
            device_id_type=MESH,
        )

    sides = ((0, i > 0), (1, i < ni - 1))

    def send_halo(number, chunk):
        for side, there in sides:
            @pl.when(there)
            def _():
                halo_copy(number, side, chunk).start()

    def wait_halo(number):
        for side, there in sides:
            @pl.when(there)
            def _():
                for chunk in range(CHUNKS):
                    halo_copy(number, 1 - side, chunk).wait_recv()

    def finish_halo(number):
        for side, there in sides:
            @pl.when(there)
            def _():
                for chunk in range(CHUNKS):
                    halo_copy(number, side, chunk).wait_send()

    def place_of(way):
        return jnp.where(way == 0, k, nk - 1 - k)

    def chain_copy(stage, way, comp):
        return pltpu.make_async_remote_copy(
            src_ref=chain_out.at[stage, way, comp],
            dst_ref=chain_in.at[stage, way, comp],
            send_sem=chain_send.at[stage, way, comp],
            recv_sem=chain_recv.at[stage, way, comp],
            device_id={"gz": k + 1 - 2 * way},
            device_id_type=MESH,
        )

    def relay(stage, way, step):
        for comp in range(comps):
            @pl.when(place_of(way) > 0)
            def _():
                chain_copy(stage, way, comp).wait_recv()

            put(chain_out, step(way, comp, get(chain_in, stage, way, comp)), stage, way, comp)

            @pl.when(place_of(way) < nk - 1)
            def _():
                chain_copy(stage, way, comp).start()

    def finish_chain(stage):
        for way, there in ((0, k < nk - 1), (1, k > 0)):
            @pl.when(there)
            def _():
                for comp in range(comps):
                    chain_copy(stage, way, comp).wait_send()

    def edge_copy(stage, way, far):
        return pltpu.make_async_remote_copy(
            src_ref=edge_out.at[stage, way],
            dst_ref=edge_in.at[stage, way, far - 1],
            send_sem=edge_send.at[stage, way, far - 1],
            recv_sem=edge_recv.at[stage, way, far - 1],
            device_id={"gz": k + far * (1 - 2 * way)},
            device_id_type=MESH,
        )

    def send_edges(stage, way, values):
        for comp in range(comps):
            for part in range(2):
                edge_out[stage, way, comp, part, :1] = values[comp][part][:1]
                edge_out[stage, way, comp, part, 1:] = values[comp][part][rows - 1:]
        for far in range(nk - 1, 0, -1):
            @pl.when(place_of(way) < nk - far)
            def _():
                edge_copy(stage, way, far).start()

    def wait_edges(stage):
        for way in range(2):
            for far in range(1, nk):
                @pl.when(place_of(way) >= far)
                def _():
                    edge_copy(stage, way, far).wait_recv()

    def finish_edges(stage):
        for way in range(2):
            for far in range(1, nk):
                @pl.when(place_of(way) < nk - far)
                def _():
                    edge_copy(stage, way, far).wait_send()

    loads[0].wait()
    for z in range(depth):
        for part in range(2):
            here = cur[z, part]
            halo_out[0, 0, z, part] = here[:, :1]
            halo_out[0, 1, z, part] = here[:, rows - 1:]

    loads[1].wait()
    loads[2].wait()
    for z in range(depth):
        sigma = look_up(conductance, conductance.shape[0], cls[z])
        real = (2.0 + 4.0 * COUPLING) + PENALTY * bnd[z].astype(jnp.float32)
        for comp in range(comps):
            diagonal = (real, sigma * strengths[comp])
            if z:
                before = get(piv, z - 1, comp)
                diagonal = (diagonal[0] - before[0], diagonal[1] - before[1])
            pivot = inverse(diagonal)
            put(piv, pivot, z, comp)
            if z == 1:
                put(vec_v, before, z, comp)
            elif z > 1:
                put(vec_v, mul(before, get(vec_v, z - 1, comp)), z, comp)
    for comp in range(comps):
        pivot = get(piv, last, comp)
        column_v, column_u = mul(pivot, get(vec_v, last, comp)), pivot
        put(vec_v, column_v, last, comp)
        put(vec_u, column_u, last, comp)
        put(ends, column_u, 1, comp)
        for z in range(last - 1, -1, -1):
            pivot = get(piv, z, comp)
            column_u = mul(pivot, column_u)
            put(vec_u, column_u, z, comp)
            if z:
                column_v = mul(pivot, add(get(vec_v, z, comp), column_v))
            else:
                column_v = mul(pivot, (1.0 + column_v[0], column_v[1]))
            put(vec_v, column_v, z, comp)
        put(ends, column_v, 0, comp)

    pl.semaphore_wait(barrier, sum(there.astype(jnp.int32) for there, _ in neighbours))
    for chunk in range(CHUNKS):
        send_halo(0, chunk)

    def coefficient_step(way, comp, arrived):
        near, far = get(ends, way, comp), get(ends, 1 - way, comp)
        across = get(vec_u, 0, comp)
        passed = mul(across, inverse(one_less(mul(near, arrived))))
        put(coef_c, passed, way, comp)
        linked = mul(passed, arrived)
        put(coef_r, linked, way, comp)
        return add(far, mul(linked, across))

    def relay_coefficients(way):
        relay(0, way, coefficient_step)
        send_edges(0, way, [get(coef_c, way, comp) for comp in range(comps)])

    def local_forcing(way, comp):
        near = get(sol, last * way, comp)
        far = get(sol, last * (1 - way), comp)
        return add(far, mul(get(coef_r, way, comp), near))

    def forcing_step(way, comp, arrived):
        return add(local_forcing(way, comp), mul(get(coef_c, way, comp), arrived))

    def send_forcing_edges(stage, way):
        send_edges(stage, way, [local_forcing(way, comp) for comp in range(comps)])

    sublane = lax.broadcasted_iota(jnp.int32, (comps, rows, lanes), 1)
    lane = lax.broadcasted_iota(jnp.int32, (comps, rows, lanes), 2)
    plane = lax.broadcasted_iota(jnp.int32, (rows, lanes), 0)

    def turned_back(vectors):
        return [
            turn[0][j] * vectors[0] + turn[1][j] * vectors[1] + turn[2][j] * vectors[2]
            for j in range(comps)
        ]

    def without_halo():
        for z in range(depth):
            for part in range(2):
                here = cur[z, part]
                up = jnp.where(sublane == 0, 0.0, pltpu.roll(here, 1, 1))
                down = jnp.where(sublane == rows - 1, 0.0, pltpu.roll(here, rows - 1, 1))
                left = jnp.where(lane == 0, 0.0, pltpu.roll(here, 1, 2))
                right = jnp.where(lane == lanes - 1, 0.0, pltpu.roll(here, lanes - 1, 2))
                driven = src[z, part] + COUPLING * ((down + up) + (right + left))
                for comp, value in enumerate(turned_back(driven)):
                    rhs[z, comp, part] = value
            forward(z, [get(rhs, z, comp) for comp in range(comps)])
        backward()

    def with_halo(number):
        for z in range(depth):
            added = []
            for part in range(2):
                outer = jnp.where(
                    sublane == 0,
                    halo_in[number, 0, z, part],
                    jnp.where(sublane == rows - 1, halo_in[number, 1, z, part], 0.0),
                )
                added.append(turned_back(COUPLING * outer))
            forward(z, [
                add(get(rhs, z, comp), (added[0][comp], added[1][comp])) for comp in range(comps)
            ])
        backward()

    def forward(z, forcings):
        for comp, forcing in enumerate(forcings):
            if z:
                forcing = add(forcing, mul(get(piv, z - 1, comp), get(sol, z - 1, comp)))
            put(sol, forcing, z, comp)

    def backward():
        for comp in range(comps):
            value = mul(get(piv, last, comp), get(sol, last, comp))
            put(sol, value, last, comp)
            for z in range(last - 1, -1, -1):
                value = mul(get(piv, z, comp), add(get(sol, z, comp), value))
                put(sol, value, z, comp)

    near_way = lax.div(k * 2, nk)
    far_way = 1 - near_way

    @pl.when(place_of(near_way) == 0)
    def _():
        relay_coefficients(near_way)

    loads[3].wait()
    for number in range(SWEEPS):
        stage = number + 1
        without_halo()
        if number == 0:
            @pl.when(place_of(near_way) > 0)
            def _():
                relay_coefficients(near_way)

        relay(stage, near_way, forcing_step)
        wait_halo(number)
        with_halo(number)
        send_forcing_edges(stage, near_way)
        if number == 0:
            relay_coefficients(far_way)
        send_forcing_edges(stage, far_way)
        relay(stage, far_way, forcing_step)

        if number == 0:
            wait_edges(0)
        wait_edges(stage)
        first_in, last_in = [], []
        for comp in range(comps):
            arrived, leaving = [], []
            for way in range(2):
                total = None
                for far in range(nk - 1, 0, -1):
                    term = get(edge_in, stage, way, far - 1, comp)
                    if total is not None:
                        term = add(term, mul(get(edge_in, 0, way, far - 1, comp), total))
                    total = term
                inner = get(chain_in, stage, way, comp)
                value = tuple(
                    jnp.where(
                        plane == 0,
                        total[part][:1],
                        jnp.where(plane == rows - 1, total[part][1:], inner[part]),
                    )
                    for part in range(2)
                )
                arrived.append(value)
                leaving.append(forcing_step(way, comp, value))
            p_in, q_in = get(chain_in, 0, 0, comp), get(chain_in, 0, 1, comp)
            p_out, q_out = get(chain_out, 0, 0, comp), get(chain_out, 0, 1, comp)
            above = add(arrived[0], mul(p_in, leaving[1]))
            below = add(arrived[1], mul(q_in, leaving[0]))
            first_in.append(mul(above, inverse(one_less(mul(q_out, p_in)))))
            last_in.append(mul(below, inverse(one_less(mul(p_out, q_in)))))
        for chunk in range(CHUNKS):
            for z in range(chunk * per, (chunk + 1) * per):
                solved = []
                for comp in range(comps):
                    value = add(
                        mul(get(vec_v, z, comp), first_in[comp]),
                        mul(get(vec_u, z, comp), last_in[comp]),
                    )
                    solved.append(add(get(sol, z, comp), value))
                for part in range(2):
                    for c in range(comps):
                        value = (
                            turn[c][0] * solved[0][part]
                            + turn[c][1] * solved[1][part]
                            + turn[c][2] * solved[2][part]
                        )
                        if stage == SWEEPS:
                            out[z, part, c] = value
                        else:
                            cur[z, part, c] = value
                            halo_out[stage, 0, z, part, c] = value[:1]
                            halo_out[stage, 1, z, part, c] = value[rows - 1:]
            if stage < SWEEPS:
                send_halo(stage, chunk)

    for number in range(SWEEPS):
        finish_halo(number)
    for stage in range(SWEEPS + 1):
        finish_chain(stage)
        finish_edges(stage)


def local(ni, nk, field, source, classes, boundary, conductance, angles, strengths):
    depth, _, comps, rows, lanes = field.shape
    block = (depth, 2, comps, rows, lanes)
    lines = (depth, comps, 2, rows, lanes)
    ends = (2, comps, 2, rows, lanes)
    vmem = lambda *shape: pltpu.VMEM(shape, jnp.float32)
    dma = lambda *shape: pltpu.SemaphoreType.DMA(shape)
    whole = pl.BlockSpec(memory_space=pltpu.HBM)
    scalars = pl.BlockSpec(memory_space=pltpu.SMEM)
    return pl.pallas_call(
        functools.partial(kernel, ni, nk),
        out_shape=pltpu.VMEM(block, jnp.float32),
        in_specs=[whole] * 4 + [scalars] * 3,
        out_specs=pl.BlockSpec(memory_space=pltpu.VMEM),
        scratch_shapes=[
            vmem(*block), vmem(*block),
            pltpu.VMEM(classes.shape, jnp.int32), pltpu.VMEM(boundary.shape, jnp.int32),
            vmem(*lines), vmem(*lines), vmem(*lines), vmem(*lines), vmem(*lines),
            vmem(*ends), vmem(*ends), vmem(*ends),
            vmem(SWEEPS, 2, depth, 2, comps, 1, lanes), vmem(SWEEPS, 2, depth, 2, comps, 1, lanes),
            vmem(SWEEPS + 1, *ends), vmem(SWEEPS + 1, *ends),
            vmem(SWEEPS + 1, 2, comps, 2, 2, lanes), vmem(SWEEPS + 1, 2, nk - 1, comps, 2, 2, lanes),
            dma(4), dma(SWEEPS, 2, CHUNKS), dma(SWEEPS, 2, CHUNKS),
            dma(SWEEPS + 1, 2, comps), dma(SWEEPS + 1, 2, comps),
            dma(SWEEPS + 1, 2, nk - 1), dma(SWEEPS + 1, 2, nk - 1),
        ],
        compiler_params=pltpu.CompilerParams(
            collective_id=0, has_side_effects=True, vmem_limit_bytes=56 * 1024 * 1024
        ),
    )(field, source, classes, boundary, conductance, angles, strengths)


def solution(mesh):
    in_specs = (
        P("gz", None, None, "xy", None),
        P("gz", None, None, "xy", None),
        P("gz", "xy", None),
        P("gz", "xy", None),
        P(),
        P(),
        P(),
    )
    out_specs = P("gz", None, None, "xy", None)
    body = functools.partial(local, mesh.shape["xy"], mesh.shape["gz"])
    return jax.shard_map(body, mesh=mesh, in_specs=in_specs, out_specs=out_specs, check_vma=False)
```

```python
import functools

import jax
import jax.numpy as jnp
from jax import lax
from jax.experimental import pallas as pl
from jax.experimental.pallas import tpu as pltpu
from jax.sharding import PartitionSpec as P

SWEEPS = 2
COUPLING = 0.1
PENALTY = 4.0
CHUNKS = 4
MESH = pl.DeviceIdType.MESH


def mul(left, right):
    return (left[0] * right[0] - left[1] * right[1], left[0] * right[1] + left[1] * right[0])


def add(left, right):
    return (left[0] + right[0], left[1] + right[1])


def inverse(value):
    weight = 1.0 / (value[0] * value[0] + value[1] * value[1])
    return (value[0] * weight, -(value[1] * weight))


def one_less(value):
    return (1.0 - value[0], -value[1])


def get(ref, *index):
    return (ref[(*index, 0)], ref[(*index, 1)])


def put(ref, value, *index):
    ref[(*index, 0)] = value[0]
    ref[(*index, 1)] = value[1]


def look_up(table_ref, count, index):
    values = [table_ref[c] for c in range(count)]
    bit = 1
    while len(values) > 1:
        odd = (index & bit) != 0
        values = [
            jnp.where(odd, values[n + 1], values[n]) if n + 1 < len(values) else values[n]
            for n in range(0, len(values), 2)
        ]
        bit *= 2
    return values[0]


def rotation(angles_ref):
    turns = [jnp.full((8, 128), angles_ref[n], jnp.float32) for n in range(3)]
    c0, c1, c2 = [jnp.cos(t)[0, 0] for t in turns]
    s0, s1, s2 = [jnp.sin(t)[0, 0] for t in turns]
    first = [[c0 * c1, -s0, c0 * s1], [s0 * c1, c0, s0 * s1], [-s1, jnp.float32(0.0), c1]]
    return [[f[0] * c2 + f[1] * s2, f[1] * c2 - f[0] * s2, f[2]] for f in first]


def kernel(
    ni, nk,
    field, source, classes, boundary, conductance, angles, strengths,
    out,
    cur, src, cls, bnd, piv, vec_v, vec_u, rhs, sol,
    ends, coef_r, coef_c,
    halo_out, halo_in, chain_out, chain_in, edge_out, edge_in,
    whole_out, whole_in,
    diag, mate_diag_out, mate_diag, mate_piv, mate_v, mate_u, mate_out, mate_in,
    load_sem, halo_send, halo_recv, chain_send, chain_recv, edge_send, edge_recv,
    diag_send, diag_recv, mate_send, mate_recv, whole_send, whole_recv,
):
    i = lax.axis_index("xy")
    k = lax.axis_index("gz")
    depth, _, comps, rows, lanes = cur.shape
    per = depth // CHUNKS
    last = depth - 1
    middle = ni // 2
    mate = ni - 1 - i

    def crossing(side):
        return i + side == middle

    paired = crossing(0) | crossing(1)
    direct = lax.rem(i, 2) == 0

    loads = [
        pltpu.make_async_copy(a, b, load_sem.at[n])
        for n, (a, b) in enumerate(((field, cur), (classes, cls), (boundary, bnd), (source, src)))
    ]
    for copy in loads:
        copy.start()

    barrier = pltpu.get_barrier_semaphore()
    neighbours = [(i > 0, {"xy": i - 1}), (i < ni - 1, {"xy": i + 1})]
    for far in range(1, nk):
        for there, target in ((k >= far, k - far), (k < nk - far, k + far)):
            neighbours += [(there, {"gz": target}), (there & paired, {"xy": mate, "gz": target})]
    for there, target in neighbours:
        @pl.when(there)
        def _():
            pl.semaphore_signal(barrier, inc=1, device_id=target, device_id_type=MESH)

    for side, alone in ((0, i == 0), (1, i == ni - 1)):
        @pl.when(alone)
        def _():
            for n in range(SWEEPS):
                halo_in[n, side] = jnp.zeros(halo_in.shape[2:], jnp.float32)

        @pl.when(crossing(side))
        def _():
            halo_in[SWEEPS - 1, side] = jnp.zeros(halo_in.shape[2:], jnp.float32)

    for way, place in ((0, k), (1, nk - 1 - k)):
        @pl.when(place == 0)
        def _():
            for n in range(SWEEPS + 1):
                chain_in[n, way] = jnp.zeros(chain_in.shape[2:], jnp.float32)

        for far in range(1, nk):
            @pl.when(place < far)
            def _():
                for n in range(SWEEPS + 2):
                    edge_in[n, way, far - 1] = jnp.zeros(edge_in.shape[3:], jnp.float32)
                whole_in[1, way, far - 1] = jnp.zeros(whole_in.shape[3:], jnp.float32)

            @pl.when(place <= far)
            def _():
                whole_in[0, way, far - 1] = jnp.zeros(whole_in.shape[3:], jnp.float32)

    turn = rotation(angles)

    def halo_copy(number, slot, side, chunk):
        part = pl.ds(chunk * per, per)
        return pltpu.make_async_remote_copy(
            src_ref=halo_out.at[number, side, part],
            dst_ref=halo_in.at[slot, 1 - side, part],
            send_sem=halo_send.at[number, side, chunk],
            recv_sem=halo_recv.at[slot, 1 - side, chunk],
            device_id={"xy": i + 2 * side - 1},
            device_id_type=MESH,
        )

    sides = ((0, i > 0), (1, i < ni - 1))

    def slot_of(number, side):
        if number < SWEEPS - 1:
            return number
        return number + crossing(side).astype(jnp.int32)

    def send_halo(number, chunk):
        for side, there in sides:
            @pl.when(there)
            def _():
                halo_copy(number, slot_of(number, side), side, chunk).start()

    def wait_slot(number, slot, side):
        for chunk in range(CHUNKS):
            halo_copy(number, slot, 1 - side, chunk).wait_recv()

    def wait_halo(number):
        for side, there in sides:
            late = crossing(side) if number == SWEEPS - 1 else False

            @pl.when(there & jnp.logical_not(late))
            def _():
                wait_slot(number, number, side)

    def finish_halo(number):
        for side, there in sides:
            @pl.when(there)
            def _():
                for chunk in range(CHUNKS):
                    halo_copy(number, slot_of(number, side), side, chunk).wait_send()

    def place_of(way):
        return jnp.where(way == 0, k, nk - 1 - k)

    def chain_copy(stage, way, comp):
        return pltpu.make_async_remote_copy(
            src_ref=chain_out.at[stage, way, comp],
            dst_ref=chain_in.at[stage, way, comp],
            send_sem=chain_send.at[stage, way, comp],
            recv_sem=chain_recv.at[stage, way, comp],
            device_id={"gz": k + 1 - 2 * way},
            device_id_type=MESH,
        )

    def relay(stage, way, step):
        for comp in range(comps):
            @pl.when(place_of(way) > 0)
            def _():
                chain_copy(stage, way, comp).wait_recv()

            put(chain_out, step(way, comp, get(chain_in, stage, way, comp)), stage, way, comp)

            @pl.when(place_of(way) < nk - 1)
            def _():
                chain_copy(stage, way, comp).start()

    def finish_chain(stage):
        for way, there in ((0, k < nk - 1), (1, k > 0)):
            @pl.when(there)
            def _():
                for comp in range(comps):
                    chain_copy(stage, way, comp).wait_send()

    def edge_copy(stage, way, far):
        return pltpu.make_async_remote_copy(
            src_ref=edge_out.at[stage, way],
            dst_ref=edge_in.at[stage, way, far - 1],
            send_sem=edge_send.at[stage, way, far - 1],
            recv_sem=edge_recv.at[stage, way, far - 1],
            device_id={"gz": k + far * (1 - 2 * way)},
            device_id_type=MESH,
        )

    def send_edges(stage, way, values):
        for comp in range(comps):
            for part in range(2):
                edge_out[stage, way, comp, part, :1] = values[comp][part][:1]
                edge_out[stage, way, comp, part, 1:] = values[comp][part][rows - 1:]
        for far in range(nk - 1, 0, -1):
            @pl.when(place_of(way) < nk - far)
            def _():
                edge_copy(stage, way, far).start()

    def wait_edges(stage):
        for way in range(2):
            for far in range(1, nk):
                @pl.when(place_of(way) >= far)
                def _():
                    edge_copy(stage, way, far).wait_recv()

    def finish_edges(stage):
        for way in range(2):
            for far in range(1, nk):
                @pl.when(place_of(way) < nk - far)
                def _():
                    edge_copy(stage, way, far).wait_send()

    def whole_copy(kind, way, far):
        return pltpu.make_async_remote_copy(
            src_ref=whole_out.at[kind, way],
            dst_ref=whole_in.at[kind, way, far - 1],
            send_sem=whole_send.at[kind, way, far - 1],
            recv_sem=whole_recv.at[kind, way, far - 1],
            device_id={"gz": k + far * (1 - 2 * way)},
            device_id_type=MESH,
        )

    def sends_whole(kind, way, far):
        place = place_of(way)
        return (place < nk - far) & (place > 0) if kind == 0 else place < nk - far

    def send_whole(kind, way, values):
        for comp in range(comps):
            put(whole_out, values[comp], kind, way, comp)
        for far in range(nk - 1, 0, -1):
            @pl.when(sends_whole(kind, way, far))
            def _():
                whole_copy(kind, way, far).start()

    def wait_whole():
        for way in range(2):
            for far in range(1, nk):
                for kind in range(2):
                    @pl.when(place_of(way) >= far + 1 - kind)
                    def _():
                        whole_copy(kind, way, far).wait_recv()

    def finish_whole():
        for way in range(2):
            for far in range(1, nk):
                for kind in range(2):
                    @pl.when(sends_whole(kind, way, far))
                    def _():
                        whole_copy(kind, way, far).wait_send()

    def diag_copy():
        return pltpu.make_async_remote_copy(
            src_ref=mate_diag_out,
            dst_ref=mate_diag,
            send_sem=diag_send,
            recv_sem=diag_recv,
            device_id={"xy": mate},
            device_id_type=MESH,
        )

    def mate_copy(way, far):
        return pltpu.make_async_remote_copy(
            src_ref=mate_out,
            dst_ref=mate_in.at[way, far - 1],
            send_sem=mate_send.at[way, far - 1],
            recv_sem=mate_recv.at[way, far - 1],
            device_id={"xy": mate, "gz": k + far * (1 - 2 * way)},
            device_id_type=MESH,
        )

    loads[0].wait()
    for z in range(depth):
        for part in range(2):
            here = cur[z, part]
            halo_out[0, 0, z, part] = here[:, :1]
            halo_out[0, 1, z, part] = here[:, rows - 1:]

    loads[1].wait()
    loads[2].wait()
    for z in range(depth):
        sigma = look_up(conductance, conductance.shape[0], cls[z])
        real = (2.0 + 4.0 * COUPLING) + PENALTY * bnd[z].astype(jnp.float32)
        put(diag, (real, sigma), z)
        for comp in range(comps):
            diagonal = (real, sigma * strengths[comp])
            if z:
                before = get(piv, z - 1, comp)
                diagonal = (diagonal[0] - before[0], diagonal[1] - before[1])
            pivot = inverse(diagonal)
            put(piv, pivot, z, comp)
            if z == 1:
                put(vec_v, before, z, comp)
            elif z > 1:
                put(vec_v, mul(before, get(vec_v, z - 1, comp)), z, comp)
    for comp in range(comps):
        pivot = get(piv, last, comp)
        column_v, column_u = mul(pivot, get(vec_v, last, comp)), pivot
        put(vec_v, column_v, last, comp)
        put(vec_u, column_u, last, comp)
        put(ends, column_u, 1, comp)
        for z in range(last - 1, -1, -1):
            pivot = get(piv, z, comp)
            column_u = mul(pivot, column_u)
            put(vec_u, column_u, z, comp)
            if z:
                column_v = mul(pivot, add(get(vec_v, z, comp), column_v))
            else:
                column_v = mul(pivot, (1.0 + column_v[0], column_v[1]))
            put(vec_v, column_v, z, comp)
        put(ends, column_v, 0, comp)

    pl.semaphore_wait(barrier, sum(there.astype(jnp.int32) for there, _ in neighbours))
    for chunk in range(CHUNKS):
        send_halo(0, chunk)
    for side in range(2):
        @pl.when(crossing(side))
        def _():
            row = side * (rows - 1)
            for z in range(depth):
                mate_diag_out[z] = diag[z, :, row:row + 1]
            diag_copy().start()

    def mate_columns():
        diag_copy().wait_recv()
        for z in range(depth):
            real, sigma = get(mate_diag, z)
            for comp in range(comps):
                diagonal = (real, sigma * strengths[comp])
                if z:
                    before = get(mate_piv, z - 1, comp)
                    diagonal = (diagonal[0] - before[0], diagonal[1] - before[1])
                put(mate_piv, inverse(diagonal), z, comp)
                if z == 1:
                    put(mate_v, before, z, comp)
                elif z > 1:
                    put(mate_v, mul(before, get(mate_v, z - 1, comp)), z, comp)
        for comp in range(comps):
            pivot = get(mate_piv, last, comp)
            column_v, column_u = mul(pivot, get(mate_v, last, comp)), pivot
            put(mate_v, column_v, last, comp)
            put(mate_u, column_u, last, comp)
            for z in range(last - 1, -1, -1):
                pivot = get(mate_piv, z, comp)
                column_u = mul(pivot, column_u)
                put(mate_u, column_u, z, comp)
                if z:
                    column_v = mul(pivot, add(get(mate_v, z, comp), column_v))
                else:
                    column_v = mul(pivot, (1.0 + column_v[0], column_v[1]))
                put(mate_v, column_v, z, comp)

    def send_to_mates(side):
        row = side * (rows - 1)
        for comp in range(comps):
            for end, column in enumerate((mate_v, mate_u)):
                total = None
                for z in range(depth):
                    ours = get(sol, z, comp)
                    term = mul(
                        get(column, z, comp), (ours[0][row:row + 1], ours[1][row:row + 1])
                    )
                    total = term if total is None else add(total, term)
                put(mate_out, (COUPLING * total[0], COUPLING * total[1]), comp, end)
        for way in range(2):
            for far in range(nk - 1, 0, -1):
                @pl.when(place_of(way) < nk - far)
                def _():
                    mate_copy(way, far).start()

    def add_from_mates(stage, side):
        for way in range(2):
            for far in range(1, nk):
                @pl.when(place_of(way) >= far)
                def _():
                    mate_copy(way, far).wait_recv()
                    for comp in range(comps):
                        near = get(mate_in, way, far - 1, comp, way)
                        beyond = get(mate_in, way, far - 1, comp, 1 - way)
                        link = get(edge_in, SWEEPS + 1, way, far - 1, comp)
                        link = (link[0][side:side + 1], link[1][side:side + 1])
                        extra = add(beyond, mul(link, near))
                        for part in range(2):
                            edge_in[stage, way, far - 1, comp, part, side:side + 1] = (
                                edge_in[stage, way, far - 1, comp, part, side:side + 1]
                                + extra[part]
                            )

    def coefficient_step(way, comp, arrived):
        near, far = get(ends, way, comp), get(ends, 1 - way, comp)
        across = get(vec_u, 0, comp)
        passed = mul(across, inverse(one_less(mul(near, arrived))))
        put(coef_c, passed, way, comp)
        linked = mul(passed, arrived)
        put(coef_r, linked, way, comp)
        return add(far, mul(linked, across))

    def relay_coefficients(way):
        relay(0, way, coefficient_step)
        send_edges(0, way, [get(coef_c, way, comp) for comp in range(comps)])

        @pl.when(paired)
        def _():
            send_edges(SWEEPS + 1, way, [get(coef_r, way, comp) for comp in range(comps)])

    def local_forcing(way, comp):
        near = get(sol, last * way, comp)
        far = get(sol, last * (1 - way), comp)
        return add(far, mul(get(coef_r, way, comp), near))

    def forcing_step(way, comp, arrived):
        return add(local_forcing(way, comp), mul(get(coef_c, way, comp), arrived))

    def send_forcing_edges(stage, way):
        send_edges(stage, way, [local_forcing(way, comp) for comp in range(comps)])

    sublane = lax.broadcasted_iota(jnp.int32, (comps, rows, lanes), 1)
    lane = lax.broadcasted_iota(jnp.int32, (comps, rows, lanes), 2)
    plane = lax.broadcasted_iota(jnp.int32, (rows, lanes), 0)

    def turned_back(vectors):
        return [
            turn[0][j] * vectors[0] + turn[1][j] * vectors[1] + turn[2][j] * vectors[2]
            for j in range(comps)
        ]

    def without_halo():
        for z in range(depth):
            for part in range(2):
                here = cur[z, part]
                up = jnp.where(sublane == 0, 0.0, pltpu.roll(here, 1, 1))
                down = jnp.where(sublane == rows - 1, 0.0, pltpu.roll(here, rows - 1, 1))
                left = jnp.where(lane == 0, 0.0, pltpu.roll(here, 1, 2))
                right = jnp.where(lane == lanes - 1, 0.0, pltpu.roll(here, lanes - 1, 2))
                driven = src[z, part] + COUPLING * ((down + up) + (right + left))
                for comp, value in enumerate(turned_back(driven)):
                    rhs[z, comp, part] = value
            forward(z, [get(rhs, z, comp) for comp in range(comps)])
        backward()

    def with_halo(above, below):
        for z in range(depth):
            added = []
            for part in range(2):
                outer = jnp.where(
                    sublane == 0,
                    halo_in[above, 0, z, part],
                    jnp.where(sublane == rows - 1, halo_in[below, 1, z, part], 0.0),
                )
                added.append(turned_back(COUPLING * outer))
            forward(z, [
                add(get(rhs, z, comp), (added[0][comp], added[1][comp])) for comp in range(comps)
            ])
        backward()

    def forward(z, forcings):
        for comp, forcing in enumerate(forcings):
            if z:
                forcing = add(forcing, mul(get(piv, z - 1, comp), get(sol, z - 1, comp)))
            put(sol, forcing, z, comp)

    def backward():
        for comp in range(comps):
            value = mul(get(piv, last, comp), get(sol, last, comp))
            put(sol, value, last, comp)
            for z in range(last - 1, -1, -1):
                value = mul(get(piv, z, comp), add(get(sol, z, comp), value))
                put(sol, value, z, comp)

    near_way = lax.div(k * 2, nk)
    far_way = 1 - near_way

    @pl.when(place_of(near_way) == 0)
    def _():
        relay_coefficients(near_way)

    loads[3].wait()
    ender = place_of(far_way) == nk - 1

    def combine_whole(stage):
        for way in range(2):
            for comp in range(comps):
                total = get(whole_in, 1, way, nk - 2, comp)
                for far in range(nk - 2, 0, -1):
                    passed = mul(get(whole_in, 0, way, far - 1, comp), total)
                    total = add(get(whole_in, 1, way, far - 1, comp), passed)
                put(chain_in, total, stage, way, comp)

    def with_mate_halo(number):
        for side in range(2):
            @pl.when(crossing(side))
            def _():
                wait_slot(number, SWEEPS, side)

        with_halo(slot_of(number, 0), slot_of(number, 1))

    for number in range(SWEEPS):
        stage = number + 1
        without_halo()
        if number == 0:
            @pl.when(place_of(near_way) > 0)
            def _():
                relay_coefficients(near_way)

            relay(stage, near_way, forcing_step)
        else:
            @pl.when(direct)
            def _():
                for way in range(2):
                    send_whole(1, way, [local_forcing(way, comp) for comp in range(comps)])

            @pl.when(jnp.logical_not(direct))
            def _():
                relay(stage, near_way, forcing_step)

        wait_halo(number)
        with_halo(number, number)
        send_forcing_edges(stage, near_way)
        if number == 0:
            @pl.when(paired & ender)
            def _():
                mate_columns()

            relay_coefficients(far_way)
            send_forcing_edges(stage, far_way)
            relay(stage, far_way, forcing_step)

            @pl.when(direct)
            def _():
                for way in range(2):
                    send_whole(0, way, [get(coef_c, way, comp) for comp in range(comps)])

            @pl.when(paired & jnp.logical_not(ender))
            def _():
                mate_columns()

            wait_edges(0)
        else:
            send_forcing_edges(stage, far_way)

            @pl.when(paired & ender)
            def _():
                with_mate_halo(number)

            @pl.when(direct)
            def _():
                wait_whole()
                combine_whole(stage)

            @pl.when(jnp.logical_not(direct))
            def _():
                relay(stage, far_way, forcing_step)

            @pl.when(paired & jnp.logical_not(ender))
            def _():
                with_mate_halo(number)

        wait_edges(stage)
        if stage == SWEEPS:
            @pl.when(paired)
            def _():
                wait_edges(SWEEPS + 1)
                for side in range(2):
                    @pl.when(crossing(side))
                    def _():
                        add_from_mates(stage, side)

        first_in, last_in = [], []
        for comp in range(comps):
            arrived, leaving = [], []
            for way in range(2):
                total = None
                for far in range(nk - 1, 0, -1):
                    term = get(edge_in, stage, way, far - 1, comp)
                    if total is not None:
                        term = add(term, mul(get(edge_in, 0, way, far - 1, comp), total))
                    total = term
                inner = get(chain_in, stage, way, comp)
                value = tuple(
                    jnp.where(
                        plane == 0,
                        total[part][:1],
                        jnp.where(plane == rows - 1, total[part][1:], inner[part]),
                    )
                    for part in range(2)
                )
                arrived.append(value)
                leaving.append(forcing_step(way, comp, value))
            p_in, q_in = get(chain_in, 0, 0, comp), get(chain_in, 0, 1, comp)
            p_out, q_out = get(chain_out, 0, 0, comp), get(chain_out, 0, 1, comp)
            above = add(arrived[0], mul(p_in, leaving[1]))
            below = add(arrived[1], mul(q_in, leaving[0]))
            first_in.append(mul(above, inverse(one_less(mul(q_out, p_in)))))
            last_in.append(mul(below, inverse(one_less(mul(p_out, q_in)))))
        for chunk in range(CHUNKS):
            for z in range(chunk * per, (chunk + 1) * per):
                solved = []
                for comp in range(comps):
                    value = add(
                        mul(get(vec_v, z, comp), first_in[comp]),
                        mul(get(vec_u, z, comp), last_in[comp]),
                    )
                    solved.append(add(get(sol, z, comp), value))
                    if stage == SWEEPS - 1:
                        put(sol, solved[comp], z, comp)
                for part in range(2):
                    for c in range(comps):
                        value = (
                            turn[c][0] * solved[0][part]
                            + turn[c][1] * solved[1][part]
                            + turn[c][2] * solved[2][part]
                        )
                        if stage == SWEEPS:
                            out[z, part, c] = value
                        else:
                            cur[z, part, c] = value
                            halo_out[stage, 0, z, part, c] = value[:1]
                            halo_out[stage, 1, z, part, c] = value[rows - 1:]
            if stage < SWEEPS:
                send_halo(stage, chunk)
        if stage == SWEEPS - 1:
            for side in range(2):
                @pl.when(crossing(side))
                def _():
                    send_to_mates(side)

    for number in range(SWEEPS):
        finish_halo(number)
    for stage in range(SWEEPS + 1):
        if stage < SWEEPS:
            finish_chain(stage)
        finish_edges(stage)

    @pl.when(direct)
    def _():
        finish_whole()

    @pl.when(jnp.logical_not(direct))
    def _():
        finish_chain(SWEEPS)

    @pl.when(paired)
    def _():
        finish_edges(SWEEPS + 1)
        diag_copy().wait_send()
        for way in range(2):
            for far in range(1, nk):
                @pl.when(place_of(way) < nk - far)
                def _():
                    mate_copy(way, far).wait_send()


def local(ni, nk, field, source, classes, boundary, conductance, angles, strengths):
    depth, _, comps, rows, lanes = field.shape
    block = (depth, 2, comps, rows, lanes)
    lines = (depth, comps, 2, rows, lanes)
    ends = (2, comps, 2, rows, lanes)
    row_lines = (depth, comps, 2, 1, lanes)
    vmem = lambda *shape: pltpu.VMEM(shape, jnp.float32)
    dma = lambda *shape: pltpu.SemaphoreType.DMA(shape)
    whole = pl.BlockSpec(memory_space=pltpu.HBM)
    scalars = pl.BlockSpec(memory_space=pltpu.SMEM)
    return pl.pallas_call(
        functools.partial(kernel, ni, nk),
        out_shape=pltpu.VMEM(block, jnp.float32),
        in_specs=[whole] * 4 + [scalars] * 3,
        out_specs=pl.BlockSpec(memory_space=pltpu.VMEM),
        scratch_shapes=[
            vmem(*block), vmem(*block),
            pltpu.VMEM(classes.shape, jnp.int32), pltpu.VMEM(boundary.shape, jnp.int32),
            vmem(*lines), vmem(*lines), vmem(*lines), vmem(*lines), vmem(*lines),
            vmem(*ends), vmem(*ends), vmem(*ends),
            vmem(SWEEPS, 2, depth, 2, comps, 1, lanes), vmem(SWEEPS + 1, 2, depth, 2, comps, 1, lanes),
            vmem(SWEEPS + 1, *ends), vmem(SWEEPS + 1, *ends),
            vmem(SWEEPS + 2, 2, comps, 2, 2, lanes), vmem(SWEEPS + 2, 2, nk - 1, comps, 2, 2, lanes),
            vmem(2, *ends), vmem(2, 2, nk - 1, *ends[1:]),
            vmem(depth, 2, rows, lanes), vmem(depth, 2, 1, lanes), vmem(depth, 2, 1, lanes),
            vmem(*row_lines), vmem(*row_lines), vmem(*row_lines),
            vmem(comps, 2, 2, 1, lanes), vmem(2, nk - 1, comps, 2, 2, 1, lanes),
            dma(4), dma(SWEEPS, 2, CHUNKS), dma(SWEEPS + 1, 2, CHUNKS),
            dma(SWEEPS + 1, 2, comps), dma(SWEEPS + 1, 2, comps),
            dma(SWEEPS + 2, 2, nk - 1), dma(SWEEPS + 2, 2, nk - 1),
            pltpu.SemaphoreType.DMA, pltpu.SemaphoreType.DMA, dma(2, nk - 1), dma(2, nk - 1),
            dma(2, 2, nk - 1), dma(2, 2, nk - 1),
        ],
        compiler_params=pltpu.CompilerParams(
            collective_id=0, has_side_effects=True, vmem_limit_bytes=56 * 1024 * 1024
        ),
    )(field, source, classes, boundary, conductance, angles, strengths)


def solution(mesh):
    in_specs = (
        P("gz", None, None, "xy", None),
        P("gz", None, None, "xy", None),
        P("gz", "xy", None),
        P("gz", "xy", None),
        P(),
        P(),
        P(),
    )
    out_specs = P("gz", None, None, "xy", None)
    body = functools.partial(local, mesh.shape["xy"], mesh.shape["gz"])
    return jax.shard_map(body, mesh=mesh, in_specs=in_specs, out_specs=out_specs, check_vma=False)
```

```python
import functools

import jax
import jax.numpy as jnp
from jax import lax
from jax.experimental import pallas as pl
from jax.experimental.pallas import tpu as pltpu
from jax.sharding import PartitionSpec as P

SWEEPS = 2
COUPLING = 0.1
PENALTY = 4.0
CHUNKS = 4
MESH = pl.DeviceIdType.MESH


def mul(left, right):
    return (left[0] * right[0] - left[1] * right[1], left[0] * right[1] + left[1] * right[0])


def add(left, right):
    return (left[0] + right[0], left[1] + right[1])


def inverse(value):
    weight = 1.0 / (value[0] * value[0] + value[1] * value[1])
    return (value[0] * weight, -(value[1] * weight))


def one_less(value):
    return (1.0 - value[0], -value[1])


def get(ref, *index):
    return (ref[(*index, 0)], ref[(*index, 1)])


def put(ref, value, *index):
    ref[(*index, 0)] = value[0]
    ref[(*index, 1)] = value[1]


def look_up(table_ref, count, index):
    values = [table_ref[c] for c in range(count)]
    bit = 1
    while len(values) > 1:
        odd = (index & bit) != 0
        values = [
            jnp.where(odd, values[n + 1], values[n]) if n + 1 < len(values) else values[n]
            for n in range(0, len(values), 2)
        ]
        bit *= 2
    return values[0]


def rotation(angles_ref):
    turns = [jnp.full((8, 128), angles_ref[n], jnp.float32) for n in range(3)]
    c0, c1, c2 = [jnp.cos(t)[0, 0] for t in turns]
    s0, s1, s2 = [jnp.sin(t)[0, 0] for t in turns]
    first = [[c0 * c1, -s0, c0 * s1], [s0 * c1, c0, s0 * s1], [-s1, jnp.float32(0.0), c1]]
    return [[f[0] * c2 + f[1] * s2, f[1] * c2 - f[0] * s2, f[2]] for f in first]


def kernel(
    ni, nk,
    field, source, classes, boundary, conductance_hbm, angles_hbm, strengths_hbm,
    out,
    conductance, angles, strengths,
    cur, src, cls, bnd, piv, vec_v, vec_u, rhs, sol,
    ends, coef_r, coef_c,
    halo_out, halo_in, chain_out, chain_in, edge_out, edge_in,
    whole_out, whole_in,
    diag, mate_diag_out, mate_diag, mate_piv, mate_v, mate_u, mate_out, mate_in,
    load_sem, halo_send, halo_recv, chain_send, chain_recv, edge_send, edge_recv,
    diag_send, diag_recv, mate_send, mate_recv, whole_send, whole_recv,
):
    i = lax.axis_index("xy")
    k = lax.axis_index("gz")
    depth, _, comps, rows, lanes = cur.shape
    per = depth // CHUNKS
    last = depth - 1
    middle = ni // 2
    mate = ni - 1 - i

    def crossing(side):
        return i + side == middle

    paired = crossing(0) | crossing(1)
    direct = lax.rem(i, 2) == 0

    barrier = pltpu.get_barrier_semaphore()
    neighbours = [(i > 0, {"xy": i - 1}), (i < ni - 1, {"xy": i + 1})]
    for far in range(1, nk):
        for there, target in ((k >= far, k - far), (k < nk - far, k + far)):
            neighbours += [(there, {"gz": target}), (there & paired, {"xy": mate, "gz": target})]
    for there, target in neighbours:
        @pl.when(there)
        def _():
            pl.semaphore_signal(barrier, inc=1, device_id=target, device_id_type=MESH)

    loads = [
        pltpu.make_async_copy(a, b, load_sem.at[n])
        for n, (a, b) in enumerate((
            (field, cur), (classes, cls), (boundary, bnd), (source, src),
            (conductance_hbm, conductance), (angles_hbm, angles), (strengths_hbm, strengths),
        ))
    ]
    for copy in loads:
        copy.start()

    for side, alone in ((0, i == 0), (1, i == ni - 1)):
        @pl.when(alone)
        def _():
            for n in range(SWEEPS):
                halo_in[n, side] = jnp.zeros(halo_in.shape[2:], jnp.float32)

        @pl.when(crossing(side))
        def _():
            halo_in[SWEEPS - 1, side] = jnp.zeros(halo_in.shape[2:], jnp.float32)

    for way, place in ((0, k), (1, nk - 1 - k)):
        @pl.when(place == 0)
        def _():
            for n in range(SWEEPS + 1):
                chain_in[n, way] = jnp.zeros(chain_in.shape[2:], jnp.float32)

        for far in range(1, nk):
            @pl.when(place < far)
            def _():
                for n in range(SWEEPS + 2):
                    edge_in[n, way, far - 1] = jnp.zeros(edge_in.shape[3:], jnp.float32)
                for n in range(1, SWEEPS + 1):
                    whole_in[n, way, far - 1] = jnp.zeros(whole_in.shape[3:], jnp.float32)

            @pl.when(place <= far)
            def _():
                whole_in[0, way, far - 1] = jnp.zeros(whole_in.shape[3:], jnp.float32)

    def halo_copy(number, slot, side, chunk):
        part = pl.ds(chunk * per, per)
        return pltpu.make_async_remote_copy(
            src_ref=halo_out.at[number, side, part],
            dst_ref=halo_in.at[slot, 1 - side, part],
            send_sem=halo_send.at[number, side, chunk],
            recv_sem=halo_recv.at[slot, 1 - side, chunk],
            device_id={"xy": i + 2 * side - 1},
            device_id_type=MESH,
        )

    sides = ((0, i > 0), (1, i < ni - 1))

    def slot_of(number, side):
        if number < SWEEPS - 1:
            return number
        return number + crossing(side).astype(jnp.int32)

    def send_halo(number, chunk):
        for side, there in sides:
            @pl.when(there)
            def _():
                halo_copy(number, slot_of(number, side), side, chunk).start()

    def wait_slot(number, slot, side):
        for chunk in range(CHUNKS):
            halo_copy(number, slot, 1 - side, chunk).wait_recv()

    def wait_halo(number):
        for side, there in sides:
            late = crossing(side) if number == SWEEPS - 1 else False

            @pl.when(there & jnp.logical_not(late))
            def _():
                wait_slot(number, number, side)

    def finish_halo(number):
        for side, there in sides:
            @pl.when(there)
            def _():
                for chunk in range(CHUNKS):
                    halo_copy(number, slot_of(number, side), side, chunk).wait_send()

    def place_of(way):
        return jnp.where(way == 0, k, nk - 1 - k)

    def chain_copy(stage, way, comp):
        return pltpu.make_async_remote_copy(
            src_ref=chain_out.at[stage, way, comp],
            dst_ref=chain_in.at[stage, way, comp],
            send_sem=chain_send.at[stage, way, comp],
            recv_sem=chain_recv.at[stage, way, comp],
            device_id={"gz": k + 1 - 2 * way},
            device_id_type=MESH,
        )

    def relay(stage, way, step):
        for comp in range(comps):
            @pl.when(place_of(way) > 0)
            def _():
                chain_copy(stage, way, comp).wait_recv()

            put(chain_out, step(way, comp, get(chain_in, stage, way, comp)), stage, way, comp)

            @pl.when(place_of(way) < nk - 1)
            def _():
                chain_copy(stage, way, comp).start()

    def finish_chain(stage):
        for way, there in ((0, k < nk - 1), (1, k > 0)):
            @pl.when(there)
            def _():
                for comp in range(comps):
                    chain_copy(stage, way, comp).wait_send()

    def edge_copy(stage, way, far):
        return pltpu.make_async_remote_copy(
            src_ref=edge_out.at[stage, way],
            dst_ref=edge_in.at[stage, way, far - 1],
            send_sem=edge_send.at[stage, way, far - 1],
            recv_sem=edge_recv.at[stage, way, far - 1],
            device_id={"gz": k + far * (1 - 2 * way)},
            device_id_type=MESH,
        )

    def send_edges(stage, way, values):
        for comp in range(comps):
            for part in range(2):
                edge_out[stage, way, comp, part, :1] = values[comp][part][:1]
                edge_out[stage, way, comp, part, 1:] = values[comp][part][rows - 1:]
        for far in range(nk - 1, 0, -1):
            @pl.when(place_of(way) < nk - far)
            def _():
                edge_copy(stage, way, far).start()

    def wait_edges(stage):
        for way in range(2):
            for far in range(1, nk):
                @pl.when(place_of(way) >= far)
                def _():
                    edge_copy(stage, way, far).wait_recv()

    def finish_edges(stage):
        for way in range(2):
            for far in range(1, nk):
                @pl.when(place_of(way) < nk - far)
                def _():
                    edge_copy(stage, way, far).wait_send()

    def whole_copy(kind, way, far):
        return pltpu.make_async_remote_copy(
            src_ref=whole_out.at[kind, way],
            dst_ref=whole_in.at[kind, way, far - 1],
            send_sem=whole_send.at[kind, way, far - 1],
            recv_sem=whole_recv.at[kind, way, far - 1],
            device_id={"gz": k + far * (1 - 2 * way)},
            device_id_type=MESH,
        )

    def sends_whole(kind, way, far):
        place = place_of(way)
        return (place < nk - far) & (place > 0) if kind == 0 else place < nk - far

    def send_whole(kind, way, values):
        for comp in range(comps):
            put(whole_out, values[comp], kind, way, comp)
        for far in range(nk - 1, 0, -1):
            @pl.when(sends_whole(kind, way, far))
            def _():
                whole_copy(kind, way, far).start()

    def wait_whole(kind):
        for way in range(2):
            for far in range(1, nk):
                @pl.when(place_of(way) >= (far if kind else far + 1))
                def _():
                    whole_copy(kind, way, far).wait_recv()

    def finish_whole():
        for way in range(2):
            for far in range(1, nk):
                for kind in (0, SWEEPS):
                    @pl.when(sends_whole(kind, way, far))
                    def _():
                        whole_copy(kind, way, far).wait_send()

    def diag_copy():
        return pltpu.make_async_remote_copy(
            src_ref=mate_diag_out,
            dst_ref=mate_diag,
            send_sem=diag_send,
            recv_sem=diag_recv,
            device_id={"xy": mate},
            device_id_type=MESH,
        )

    def mate_copy(way, far):
        return pltpu.make_async_remote_copy(
            src_ref=mate_out,
            dst_ref=mate_in.at[way, far - 1],
            send_sem=mate_send.at[way, far - 1],
            recv_sem=mate_recv.at[way, far - 1],
            device_id={"xy": mate, "gz": k + far * (1 - 2 * way)},
            device_id_type=MESH,
        )

    loads[0].wait()
    for z in range(depth):
        for part in range(2):
            here = cur[z, part]
            halo_out[0, 0, z, part] = here[:, :1]
            halo_out[0, 1, z, part] = here[:, rows - 1:]

    for n in (1, 2, 4, 6):
        loads[n].wait()
    for z in range(depth):
        sigma = look_up(conductance, conductance.shape[0], cls[z])
        real = (2.0 + 4.0 * COUPLING) + PENALTY * bnd[z].astype(jnp.float32)
        put(diag, (real, sigma), z)
        for comp in range(comps):
            diagonal = (real, sigma * strengths[comp])
            if z:
                before = get(piv, z - 1, comp)
                diagonal = (diagonal[0] - before[0], diagonal[1] - before[1])
            pivot = inverse(diagonal)
            put(piv, pivot, z, comp)
            if z == 1:
                put(vec_v, before, z, comp)
            elif z > 1:
                put(vec_v, mul(before, get(vec_v, z - 1, comp)), z, comp)
    for comp in range(comps):
        pivot = get(piv, last, comp)
        column_v, column_u = mul(pivot, get(vec_v, last, comp)), pivot
        put(vec_v, column_v, last, comp)
        put(vec_u, column_u, last, comp)
        put(ends, column_u, 1, comp)
        for z in range(last - 1, -1, -1):
            pivot = get(piv, z, comp)
            column_u = mul(pivot, column_u)
            put(vec_u, column_u, z, comp)
            if z:
                column_v = mul(pivot, add(get(vec_v, z, comp), column_v))
            else:
                column_v = mul(pivot, (1.0 + column_v[0], column_v[1]))
            put(vec_v, column_v, z, comp)
        put(ends, column_v, 0, comp)

    pl.semaphore_wait(barrier, sum(there.astype(jnp.int32) for there, _ in neighbours))
    for chunk in range(CHUNKS):
        send_halo(0, chunk)
    for side in range(2):
        @pl.when(crossing(side))
        def _():
            row = side * (rows - 1)
            for z in range(depth):
                mate_diag_out[z] = diag[z, :, row:row + 1]
            diag_copy().start()

    def mate_columns():
        diag_copy().wait_recv()
        for z in range(depth):
            real, sigma = get(mate_diag, z)
            for comp in range(comps):
                diagonal = (real, sigma * strengths[comp])
                if z:
                    before = get(mate_piv, z - 1, comp)
                    diagonal = (diagonal[0] - before[0], diagonal[1] - before[1])
                put(mate_piv, inverse(diagonal), z, comp)
                if z == 1:
                    put(mate_v, before, z, comp)
                elif z > 1:
                    put(mate_v, mul(before, get(mate_v, z - 1, comp)), z, comp)
        for comp in range(comps):
            pivot = get(mate_piv, last, comp)
            column_v, column_u = mul(pivot, get(mate_v, last, comp)), pivot
            put(mate_v, column_v, last, comp)
            put(mate_u, column_u, last, comp)
            for z in range(last - 1, -1, -1):
                pivot = get(mate_piv, z, comp)
                column_u = mul(pivot, column_u)
                put(mate_u, column_u, z, comp)
                if z:
                    column_v = mul(pivot, add(get(mate_v, z, comp), column_v))
                else:
                    column_v = mul(pivot, (1.0 + column_v[0], column_v[1]))
                put(mate_v, column_v, z, comp)

    def send_to_mates(side):
        row = side * (rows - 1)
        for comp in range(comps):
            for end, column in enumerate((mate_v, mate_u)):
                total = None
                for z in range(depth):
                    ours = get(sol, z, comp)
                    term = mul(
                        get(column, z, comp), (ours[0][row:row + 1], ours[1][row:row + 1])
                    )
                    total = term if total is None else add(total, term)
                put(mate_out, (COUPLING * total[0], COUPLING * total[1]), comp, end)
        for way in range(2):
            for far in range(nk - 1, 0, -1):
                @pl.when(place_of(way) < nk - far)
                def _():
                    mate_copy(way, far).start()

    def add_from_mates(stage, side):
        for way in range(2):
            for far in range(1, nk):
                @pl.when(place_of(way) >= far)
                def _():
                    mate_copy(way, far).wait_recv()
                    for comp in range(comps):
                        near = get(mate_in, way, far - 1, comp, way)
                        beyond = get(mate_in, way, far - 1, comp, 1 - way)
                        link = get(edge_in, SWEEPS + 1, way, far - 1, comp)
                        link = (link[0][side:side + 1], link[1][side:side + 1])
                        extra = add(beyond, mul(link, near))
                        for part in range(2):
                            edge_in[stage, way, far - 1, comp, part, side:side + 1] = (
                                edge_in[stage, way, far - 1, comp, part, side:side + 1]
                                + extra[part]
                            )

    def coefficient_step(way, comp, arrived):
        near, far = get(ends, way, comp), get(ends, 1 - way, comp)
        across = get(vec_u, 0, comp)
        passed = mul(across, inverse(one_less(mul(near, arrived))))
        put(coef_c, passed, way, comp)
        linked = mul(passed, arrived)
        put(coef_r, linked, way, comp)
        return add(far, mul(linked, across))

    def relay_coefficients(way):
        relay(0, way, coefficient_step)
        send_edges(0, way, [get(coef_c, way, comp) for comp in range(comps)])

        @pl.when(paired)
        def _():
            send_edges(SWEEPS + 1, way, [get(coef_r, way, comp) for comp in range(comps)])

    def local_forcing(way, comp):
        near = get(sol, last * way, comp)
        far = get(sol, last * (1 - way), comp)
        return add(far, mul(get(coef_r, way, comp), near))

    def forcing_step(way, comp, arrived):
        return add(local_forcing(way, comp), mul(get(coef_c, way, comp), arrived))

    def send_forcing_edges(stage, way):
        send_edges(stage, way, [local_forcing(way, comp) for comp in range(comps)])

    sublane = lax.broadcasted_iota(jnp.int32, (comps, rows, lanes), 1)
    lane = lax.broadcasted_iota(jnp.int32, (comps, rows, lanes), 2)
    plane = lax.broadcasted_iota(jnp.int32, (rows, lanes), 0)

    def turned_back(vectors):
        return [
            turn[0][j] * vectors[0] + turn[1][j] * vectors[1] + turn[2][j] * vectors[2]
            for j in range(comps)
        ]

    def without_halo():
        for z in range(depth):
            for part in range(2):
                here = cur[z, part]
                up = jnp.where(sublane == 0, 0.0, pltpu.roll(here, 1, 1))
                down = jnp.where(sublane == rows - 1, 0.0, pltpu.roll(here, rows - 1, 1))
                left = jnp.where(lane == 0, 0.0, pltpu.roll(here, 1, 2))
                right = jnp.where(lane == lanes - 1, 0.0, pltpu.roll(here, lanes - 1, 2))
                driven = src[z, part] + COUPLING * ((down + up) + (right + left))
                for comp, value in enumerate(turned_back(driven)):
                    rhs[z, comp, part] = value
            forward(z, [get(rhs, z, comp) for comp in range(comps)])
        backward()

    def with_halo(above, below):
        for z in range(depth):
            added = []
            for part in range(2):
                outer = jnp.where(
                    sublane == 0,
                    halo_in[above, 0, z, part],
                    jnp.where(sublane == rows - 1, halo_in[below, 1, z, part], 0.0),
                )
                added.append(turned_back(COUPLING * outer))
            forward(z, [
                add(get(rhs, z, comp), (added[0][comp], added[1][comp])) for comp in range(comps)
            ])
        backward()

    def forward(z, forcings):
        for comp, forcing in enumerate(forcings):
            if z:
                forcing = add(forcing, mul(get(piv, z - 1, comp), get(sol, z - 1, comp)))
            put(sol, forcing, z, comp)

    def backward():
        for comp in range(comps):
            value = mul(get(piv, last, comp), get(sol, last, comp))
            put(sol, value, last, comp)
            for z in range(last - 1, -1, -1):
                value = mul(get(piv, z, comp), add(get(sol, z, comp), value))
                put(sol, value, z, comp)

    near_way = lax.div(k * 2, nk)
    far_way = 1 - near_way

    @pl.when(place_of(near_way) == 0)
    def _():
        relay_coefficients(near_way)

    loads[3].wait()
    loads[5].wait()
    turn = rotation(angles)
    ender = place_of(far_way) == nk - 1

    def combine_whole(stage):
        for way in range(2):
            for comp in range(comps):
                total = get(whole_in, stage, way, nk - 2, comp)
                for far in range(nk - 2, 0, -1):
                    passed = mul(get(whole_in, 0, way, far - 1, comp), total)
                    total = add(get(whole_in, stage, way, far - 1, comp), passed)
                put(chain_in, total, stage, way, comp)

    def with_mate_halo(number):
        for side in range(2):
            @pl.when(crossing(side))
            def _():
                wait_slot(number, SWEEPS, side)

        with_halo(slot_of(number, 0), slot_of(number, 1))

    def far_first():
        relay_coefficients(far_way)
        relay(1, far_way, forcing_step)

    early = paired & jnp.logical_not(ender)
    for number in range(SWEEPS):
        stage = number + 1
        without_halo()
        if number == 0:
            @pl.when(place_of(near_way) > 0)
            def _():
                relay_coefficients(near_way)

            relay(stage, near_way, forcing_step)

            @pl.when(early)
            def _():
                far_first()
        else:
            @pl.when(direct)
            def _():
                for way in range(2):
                    send_whole(stage, way, [local_forcing(way, comp) for comp in range(comps)])

            @pl.when(jnp.logical_not(direct))
            def _():
                relay(stage, near_way, forcing_step)

        wait_halo(number)
        with_halo(number, number)
        send_forcing_edges(stage, near_way)
        if number == 0:
            @pl.when(paired & ender)
            def _():
                mate_columns()

            @pl.when(jnp.logical_not(early))
            def _():
                far_first()

            send_forcing_edges(stage, far_way)

            @pl.when(direct)
            def _():
                for way in range(2):
                    send_whole(0, way, [get(coef_c, way, comp) for comp in range(comps)])

            @pl.when(paired & jnp.logical_not(ender))
            def _():
                mate_columns()

            wait_edges(0)
        else:
            send_forcing_edges(stage, far_way)

            @pl.when(paired & ender)
            def _():
                with_mate_halo(number)

            @pl.when(direct)
            def _():
                wait_whole(0)
                wait_whole(stage)
                combine_whole(stage)

            @pl.when(jnp.logical_not(direct))
            def _():
                relay(stage, far_way, forcing_step)

            @pl.when(paired & jnp.logical_not(ender))
            def _():
                with_mate_halo(number)

        wait_edges(stage)
        if stage == SWEEPS:
            @pl.when(paired)
            def _():
                wait_edges(SWEEPS + 1)
                for side in range(2):
                    @pl.when(crossing(side))
                    def _():
                        add_from_mates(stage, side)

        first_in, last_in = [], []
        for comp in range(comps):
            arrived, leaving = [], []
            for way in range(2):
                total = None
                for far in range(nk - 1, 0, -1):
                    term = get(edge_in, stage, way, far - 1, comp)
                    if total is not None:
                        term = add(term, mul(get(edge_in, 0, way, far - 1, comp), total))
                    total = term
                inner = get(chain_in, stage, way, comp)
                value = tuple(
                    jnp.where(
                        plane == 0,
                        total[part][:1],
                        jnp.where(plane == rows - 1, total[part][1:], inner[part]),
                    )
                    for part in range(2)
                )
                arrived.append(value)
                leaving.append(forcing_step(way, comp, value))
            p_in, q_in = get(chain_in, 0, 0, comp), get(chain_in, 0, 1, comp)
            p_out, q_out = get(chain_out, 0, 0, comp), get(chain_out, 0, 1, comp)
            above = add(arrived[0], mul(p_in, leaving[1]))
            below = add(arrived[1], mul(q_in, leaving[0]))
            first_in.append(mul(above, inverse(one_less(mul(q_out, p_in)))))
            last_in.append(mul(below, inverse(one_less(mul(p_out, q_in)))))
        for chunk in range(CHUNKS):
            for z in range(chunk * per, (chunk + 1) * per):
                solved = []
                for comp in range(comps):
                    value = add(
                        mul(get(vec_v, z, comp), first_in[comp]),
                        mul(get(vec_u, z, comp), last_in[comp]),
                    )
                    solved.append(add(get(sol, z, comp), value))
                    if stage == SWEEPS - 1:
                        put(sol, solved[comp], z, comp)
                for part in range(2):
                    for c in range(comps):
                        value = (
                            turn[c][0] * solved[0][part]
                            + turn[c][1] * solved[1][part]
                            + turn[c][2] * solved[2][part]
                        )
                        if stage == SWEEPS:
                            out[z, part, c] = value
                        else:
                            cur[z, part, c] = value
                            halo_out[stage, 0, z, part, c] = value[:1]
                            halo_out[stage, 1, z, part, c] = value[rows - 1:]
            if stage < SWEEPS:
                send_halo(stage, chunk)
        if stage == SWEEPS - 1:
            for side in range(2):
                @pl.when(crossing(side))
                def _():
                    send_to_mates(side)

    for number in range(SWEEPS):
        finish_halo(number)
    for stage in range(SWEEPS + 1):
        finish_edges(stage)
    for stage in range(SWEEPS):
        finish_chain(stage)

    @pl.when(direct)
    def _():
        finish_whole()

    @pl.when(jnp.logical_not(direct))
    def _():
        finish_chain(SWEEPS)

    @pl.when(paired)
    def _():
        finish_edges(SWEEPS + 1)
        diag_copy().wait_send()
        for way in range(2):
            for far in range(1, nk):
                @pl.when(place_of(way) < nk - far)
                def _():
                    mate_copy(way, far).wait_send()


def local(ni, nk, field, source, classes, boundary, conductance, angles, strengths):
    depth, _, comps, rows, lanes = field.shape
    block = (depth, 2, comps, rows, lanes)
    lines = (depth, comps, 2, rows, lanes)
    ends = (2, comps, 2, rows, lanes)
    row_lines = (depth, comps, 2, 1, lanes)
    vmem = lambda *shape: pltpu.VMEM(shape, jnp.float32)
    dma = lambda *shape: pltpu.SemaphoreType.DMA(shape)
    whole = pl.BlockSpec(memory_space=pltpu.HBM)
    return pl.pallas_call(
        functools.partial(kernel, ni, nk),
        out_shape=pltpu.VMEM(block, jnp.float32),
        in_specs=[whole] * 7,
        out_specs=pl.BlockSpec(memory_space=pltpu.VMEM),
        scratch_shapes=[
            *[pltpu.SMEM(v.shape, jnp.float32) for v in (conductance, angles, strengths)],
            vmem(*block), vmem(*block),
            pltpu.VMEM(classes.shape, jnp.int32), pltpu.VMEM(boundary.shape, jnp.int32),
            vmem(*lines), vmem(*lines), vmem(*lines), vmem(*lines), vmem(*lines),
            vmem(*ends), vmem(*ends), vmem(*ends),
            vmem(SWEEPS, 2, depth, 2, comps, 1, lanes), vmem(SWEEPS + 1, 2, depth, 2, comps, 1, lanes),
            vmem(SWEEPS + 1, *ends), vmem(SWEEPS + 1, *ends),
            vmem(SWEEPS + 2, 2, comps, 2, 2, lanes), vmem(SWEEPS + 2, 2, nk - 1, comps, 2, 2, lanes),
            vmem(SWEEPS + 1, *ends), vmem(SWEEPS + 1, 2, nk - 1, *ends[1:]),
            vmem(depth, 2, rows, lanes), vmem(depth, 2, 1, lanes), vmem(depth, 2, 1, lanes),
            vmem(*row_lines), vmem(*row_lines), vmem(*row_lines),
            vmem(comps, 2, 2, 1, lanes), vmem(2, nk - 1, comps, 2, 2, 1, lanes),
            dma(7), dma(SWEEPS, 2, CHUNKS), dma(SWEEPS + 1, 2, CHUNKS),
            dma(SWEEPS + 1, 2, comps), dma(SWEEPS + 1, 2, comps),
            dma(SWEEPS + 2, 2, nk - 1), dma(SWEEPS + 2, 2, nk - 1),
            pltpu.SemaphoreType.DMA, pltpu.SemaphoreType.DMA, dma(2, nk - 1), dma(2, nk - 1),
            dma(SWEEPS + 1, 2, nk - 1), dma(SWEEPS + 1, 2, nk - 1),
        ],
        compiler_params=pltpu.CompilerParams(
            collective_id=0, has_side_effects=True, vmem_limit_bytes=56 * 1024 * 1024
        ),
    )(field, source, classes, boundary, conductance, angles, strengths)


def solution(mesh):
    in_specs = (
        P("gz", None, None, "xy", None),
        P("gz", None, None, "xy", None),
        P("gz", "xy", None),
        P("gz", "xy", None),
        P(),
        P(),
        P(),
    )
    out_specs = P("gz", None, None, "xy", None)
    body = functools.partial(local, mesh.shape["xy"], mesh.shape["gz"])
    return jax.shard_map(body, mesh=mesh, in_specs=in_specs, out_specs=out_specs, check_vma=False)
```

```python
import functools

import jax
import jax.numpy as jnp
from jax import lax
from jax.experimental import pallas as pl
from jax.experimental.pallas import tpu as pltpu
from jax.sharding import PartitionSpec as P

SWEEPS = 2
COUPLING = 0.1
PENALTY = 4.0
CHUNKS = 4
MESH = pl.DeviceIdType.MESH


def mul(left, right):
    return (left[0] * right[0] - left[1] * right[1], left[0] * right[1] + left[1] * right[0])


def add(left, right):
    return (left[0] + right[0], left[1] + right[1])


def inverse(value):
    weight = 1.0 / (value[0] * value[0] + value[1] * value[1])
    return (value[0] * weight, -(value[1] * weight))


def one_less(value):
    return (1.0 - value[0], -value[1])


def get(ref, *index):
    return (ref[(*index, 0)], ref[(*index, 1)])


def put(ref, value, *index):
    ref[(*index, 0)] = value[0]
    ref[(*index, 1)] = value[1]


def look_up(table_ref, count, index):
    values = [table_ref[c] for c in range(count)]
    bit = 1
    while len(values) > 1:
        odd = (index & bit) != 0
        values = [
            jnp.where(odd, values[n + 1], values[n]) if n + 1 < len(values) else values[n]
            for n in range(0, len(values), 2)
        ]
        bit *= 2
    return values[0]


def rotation(angles_ref):
    turns = [jnp.full((8, 128), angles_ref[n], jnp.float32) for n in range(3)]
    c0, c1, c2 = [jnp.cos(t)[0, 0] for t in turns]
    s0, s1, s2 = [jnp.sin(t)[0, 0] for t in turns]
    first = [[c0 * c1, -s0, c0 * s1], [s0 * c1, c0, s0 * s1], [-s1, jnp.float32(0.0), c1]]
    return [[f[0] * c2 + f[1] * s2, f[1] * c2 - f[0] * s2, f[2]] for f in first]


def kernel(
    ni, nk,
    field, source, classes, boundary, conductance_hbm, angles_hbm, strengths_hbm,
    out,
    conductance, angles, strengths,
    cur, src, cls, bnd, piv, vec_v, vec_u, rhs, sol,
    ends, coef_r, coef_c,
    halo_out, halo_in, chain_out, chain_in, edge_out, edge_in,
    whole_out, whole_in,
    diag, mate_diag_out, mate_diag, mate_piv, mate_v, mate_u, mate_out, mate_in,
    load_sem, halo_send, halo_recv, chain_send, chain_recv, edge_send, edge_recv,
    diag_send, diag_recv, mate_send, mate_recv, whole_send, whole_recv,
):
    i = lax.axis_index("xy")
    k = lax.axis_index("gz")
    depth, _, comps, rows, lanes = cur.shape
    per = depth // CHUNKS
    last = depth - 1
    middle = ni // 2
    mate = ni - 1 - i

    def crossing(side):
        return i + side == middle

    paired = crossing(0) | crossing(1)
    direct = (lax.rem(i, 2) == 0) & jnp.logical_not(paired)

    barrier = pltpu.get_barrier_semaphore()
    neighbours = [(i > 0, {"xy": i - 1}), (i < ni - 1, {"xy": i + 1})]
    for far in range(1, nk):
        for there, target in ((k >= far, k - far), (k < nk - far, k + far)):
            neighbours += [(there, {"gz": target}), (there & paired, {"xy": mate, "gz": target})]
    for there, target in neighbours:
        @pl.when(there)
        def _():
            pl.semaphore_signal(barrier, inc=1, device_id=target, device_id_type=MESH)

    loads = [
        pltpu.make_async_copy(a, b, load_sem.at[n])
        for n, (a, b) in enumerate((
            (field, cur), (classes, cls), (boundary, bnd), (source, src),
            (conductance_hbm, conductance), (angles_hbm, angles), (strengths_hbm, strengths),
        ))
    ]
    for copy in loads:
        copy.start()

    for side, alone in ((0, i == 0), (1, i == ni - 1)):
        @pl.when(alone)
        def _():
            for n in range(SWEEPS):
                halo_in[n, side] = jnp.zeros(halo_in.shape[2:], jnp.float32)

        @pl.when(crossing(side))
        def _():
            halo_in[SWEEPS - 1, side] = jnp.zeros(halo_in.shape[2:], jnp.float32)

    for way, place in ((0, k), (1, nk - 1 - k)):
        @pl.when(place == 0)
        def _():
            for n in range(SWEEPS + 1):
                chain_in[n, way] = jnp.zeros(chain_in.shape[2:], jnp.float32)

        for far in range(1, nk):
            @pl.when(place < far)
            def _():
                for n in range(SWEEPS + 2):
                    edge_in[n, way, far - 1] = jnp.zeros(edge_in.shape[3:], jnp.float32)
                for n in range(1, SWEEPS + 1):
                    whole_in[n, way, far - 1] = jnp.zeros(whole_in.shape[3:], jnp.float32)

            @pl.when(place <= far)
            def _():
                whole_in[0, way, far - 1] = jnp.zeros(whole_in.shape[3:], jnp.float32)

    def halo_copy(number, slot, side, chunk):
        part = pl.ds(chunk * per, per)
        return pltpu.make_async_remote_copy(
            src_ref=halo_out.at[number, side, part],
            dst_ref=halo_in.at[slot, 1 - side, part],
            send_sem=halo_send.at[number, side, chunk],
            recv_sem=halo_recv.at[slot, 1 - side, chunk],
            device_id={"xy": i + 2 * side - 1},
            device_id_type=MESH,
        )

    sides = ((0, i > 0), (1, i < ni - 1))

    def slot_of(number, side):
        if number < SWEEPS - 1:
            return number
        return number + crossing(side).astype(jnp.int32)

    def send_halo(number, chunk):
        for side, there in sides:
            @pl.when(there)
            def _():
                halo_copy(number, slot_of(number, side), side, chunk).start()

    def wait_slot(number, slot, side):
        for chunk in range(CHUNKS):
            halo_copy(number, slot, 1 - side, chunk).wait_recv()

    def wait_halo(number):
        for side, there in sides:
            late = crossing(side) if number == SWEEPS - 1 else False

            @pl.when(there & jnp.logical_not(late))
            def _():
                wait_slot(number, number, side)

    def finish_halo(number):
        for side, there in sides:
            @pl.when(there)
            def _():
                for chunk in range(CHUNKS):
                    halo_copy(number, slot_of(number, side), side, chunk).wait_send()

    def place_of(way):
        return jnp.where(way == 0, k, nk - 1 - k)

    def chain_copy(stage, way, comp):
        return pltpu.make_async_remote_copy(
            src_ref=chain_out.at[stage, way, comp],
            dst_ref=chain_in.at[stage, way, comp],
            send_sem=chain_send.at[stage, way, comp],
            recv_sem=chain_recv.at[stage, way, comp],
            device_id={"gz": k + 1 - 2 * way},
            device_id_type=MESH,
        )

    def relay(stage, way, step):
        for comp in range(comps):
            @pl.when(place_of(way) > 0)
            def _():
                chain_copy(stage, way, comp).wait_recv()

            put(chain_out, step(way, comp, get(chain_in, stage, way, comp)), stage, way, comp)

            @pl.when(place_of(way) < nk - 1)
            def _():
                chain_copy(stage, way, comp).start()

    def finish_chain(stage):
        for way, there in ((0, k < nk - 1), (1, k > 0)):
            @pl.when(there)
            def _():
                for comp in range(comps):
                    chain_copy(stage, way, comp).wait_send()

    def edge_copy(stage, way, far):
        return pltpu.make_async_remote_copy(
            src_ref=edge_out.at[stage, way],
            dst_ref=edge_in.at[stage, way, far - 1],
            send_sem=edge_send.at[stage, way, far - 1],
            recv_sem=edge_recv.at[stage, way, far - 1],
            device_id={"gz": k + far * (1 - 2 * way)},
            device_id_type=MESH,
        )

    def send_edges(stage, way, values):
        for comp in range(comps):
            for part in range(2):
                edge_out[stage, way, comp, part, :1] = values[comp][part][:1]
                edge_out[stage, way, comp, part, 1:] = values[comp][part][rows - 1:]
        for far in range(nk - 1, 0, -1):
            @pl.when(place_of(way) < nk - far)
            def _():
                edge_copy(stage, way, far).start()

    def wait_edges(stage):
        for way in range(2):
            for far in range(1, nk):
                @pl.when(place_of(way) >= far)
                def _():
                    edge_copy(stage, way, far).wait_recv()

    def finish_edges(stage):
        for way in range(2):
            for far in range(1, nk):
                @pl.when(place_of(way) < nk - far)
                def _():
                    edge_copy(stage, way, far).wait_send()

    def whole_copy(kind, way, far):
        return pltpu.make_async_remote_copy(
            src_ref=whole_out.at[kind, way],
            dst_ref=whole_in.at[kind, way, far - 1],
            send_sem=whole_send.at[kind, way, far - 1],
            recv_sem=whole_recv.at[kind, way, far - 1],
            device_id={"gz": k + far * (1 - 2 * way)},
            device_id_type=MESH,
        )

    def sends_whole(kind, way, far):
        place = place_of(way)
        return (place < nk - far) & (place > 0) if kind == 0 else place < nk - far

    def send_whole(kind, way, values):
        for comp in range(comps):
            put(whole_out, values[comp], kind, way, comp)
        for far in range(nk - 1, 0, -1):
            @pl.when(sends_whole(kind, way, far))
            def _():
                whole_copy(kind, way, far).start()

    def wait_whole(kind):
        for way in range(2):
            for far in range(1, nk):
                @pl.when(place_of(way) >= (far if kind else far + 1))
                def _():
                    whole_copy(kind, way, far).wait_recv()

    def finish_whole():
        for way in range(2):
            for far in range(1, nk):
                for kind in (0, SWEEPS):
                    @pl.when(sends_whole(kind, way, far))
                    def _():
                        whole_copy(kind, way, far).wait_send()

    def diag_copy():
        return pltpu.make_async_remote_copy(
            src_ref=mate_diag_out,
            dst_ref=mate_diag,
            send_sem=diag_send,
            recv_sem=diag_recv,
            device_id={"xy": mate},
            device_id_type=MESH,
        )

    def mate_copy(way, far):
        return pltpu.make_async_remote_copy(
            src_ref=mate_out,
            dst_ref=mate_in.at[way, far - 1],
            send_sem=mate_send.at[way, far - 1],
            recv_sem=mate_recv.at[way, far - 1],
            device_id={"xy": mate, "gz": k + far * (1 - 2 * way)},
            device_id_type=MESH,
        )

    loads[0].wait()
    for z in range(depth):
        for part in range(2):
            here = cur[z, part]
            halo_out[0, 0, z, part] = here[:, :1]
            halo_out[0, 1, z, part] = here[:, rows - 1:]

    for n in (1, 2, 4, 6):
        loads[n].wait()
    for z in range(depth):
        sigma = look_up(conductance, conductance.shape[0], cls[z])
        real = (2.0 + 4.0 * COUPLING) + PENALTY * bnd[z].astype(jnp.float32)
        put(diag, (real, sigma), z)
        for comp in range(comps):
            diagonal = (real, sigma * strengths[comp])
            if z:
                before = get(piv, z - 1, comp)
                diagonal = (diagonal[0] - before[0], diagonal[1] - before[1])
            pivot = inverse(diagonal)
            put(piv, pivot, z, comp)
            if z == 1:
                put(vec_v, before, z, comp)
            elif z > 1:
                put(vec_v, mul(before, get(vec_v, z - 1, comp)), z, comp)
    for comp in range(comps):
        pivot = get(piv, last, comp)
        column_v, column_u = mul(pivot, get(vec_v, last, comp)), pivot
        put(vec_v, column_v, last, comp)
        put(vec_u, column_u, last, comp)
        put(ends, column_u, 1, comp)
        for z in range(last - 1, -1, -1):
            pivot = get(piv, z, comp)
            column_u = mul(pivot, column_u)
            put(vec_u, column_u, z, comp)
            if z:
                column_v = mul(pivot, add(get(vec_v, z, comp), column_v))
            else:
                column_v = mul(pivot, (1.0 + column_v[0], column_v[1]))
            put(vec_v, column_v, z, comp)
        put(ends, column_v, 0, comp)

    pl.semaphore_wait(barrier, sum(there.astype(jnp.int32) for there, _ in neighbours))
    for chunk in range(CHUNKS):
        send_halo(0, chunk)
    for side in range(2):
        @pl.when(crossing(side))
        def _():
            row = side * (rows - 1)
            for z in range(depth):
                mate_diag_out[z] = diag[z, :, row:row + 1]
            diag_copy().start()

    def mate_columns():
        diag_copy().wait_recv()
        for z in range(depth):
            real, sigma = get(mate_diag, z)
            for comp in range(comps):
                diagonal = (real, sigma * strengths[comp])
                if z:
                    before = get(mate_piv, z - 1, comp)
                    diagonal = (diagonal[0] - before[0], diagonal[1] - before[1])
                put(mate_piv, inverse(diagonal), z, comp)
                if z == 1:
                    put(mate_v, before, z, comp)
                elif z > 1:
                    put(mate_v, mul(before, get(mate_v, z - 1, comp)), z, comp)
        for comp in range(comps):
            pivot = get(mate_piv, last, comp)
            column_v, column_u = mul(pivot, get(mate_v, last, comp)), pivot
            put(mate_v, column_v, last, comp)
            put(mate_u, column_u, last, comp)
            for z in range(last - 1, -1, -1):
                pivot = get(mate_piv, z, comp)
                column_u = mul(pivot, column_u)
                put(mate_u, column_u, z, comp)
                if z:
                    column_v = mul(pivot, add(get(mate_v, z, comp), column_v))
                else:
                    column_v = mul(pivot, (1.0 + column_v[0], column_v[1]))
                put(mate_v, column_v, z, comp)

    def send_to_mates(side):
        row = side * (rows - 1)
        for comp in range(comps):
            for end, column in enumerate((mate_v, mate_u)):
                total = None
                for z in range(depth):
                    ours = get(sol, z, comp)
                    term = mul(
                        get(column, z, comp), (ours[0][row:row + 1], ours[1][row:row + 1])
                    )
                    total = term if total is None else add(total, term)
                put(mate_out, (COUPLING * total[0], COUPLING * total[1]), comp, end)
        for way in range(2):
            for far in range(nk - 1, 0, -1):
                @pl.when(place_of(way) < nk - far)
                def _():
                    mate_copy(way, far).start()

    def add_from_mates(stage, side):
        for way in range(2):
            for far in range(1, nk):
                @pl.when(place_of(way) >= far)
                def _():
                    mate_copy(way, far).wait_recv()
                    for comp in range(comps):
                        near = get(mate_in, way, far - 1, comp, way)
                        beyond = get(mate_in, way, far - 1, comp, 1 - way)
                        link = get(edge_in, SWEEPS + 1, way, far - 1, comp)
                        link = (link[0][side:side + 1], link[1][side:side + 1])
                        extra = add(beyond, mul(link, near))
                        for part in range(2):
                            edge_in[stage, way, far - 1, comp, part, side:side + 1] = (
                                edge_in[stage, way, far - 1, comp, part, side:side + 1]
                                + extra[part]
                            )

    def coefficient_step(way, comp, arrived):
        near, far = get(ends, way, comp), get(ends, 1 - way, comp)
        across = get(vec_u, 0, comp)
        passed = mul(across, inverse(one_less(mul(near, arrived))))
        put(coef_c, passed, way, comp)
        linked = mul(passed, arrived)
        put(coef_r, linked, way, comp)
        return add(far, mul(linked, across))

    def relay_coefficients(way):
        relay(0, way, coefficient_step)
        send_edges(0, way, [get(coef_c, way, comp) for comp in range(comps)])

        @pl.when(paired)
        def _():
            send_edges(SWEEPS + 1, way, [get(coef_r, way, comp) for comp in range(comps)])

    def local_forcing(way, comp):
        near = get(sol, last * way, comp)
        far = get(sol, last * (1 - way), comp)
        return add(far, mul(get(coef_r, way, comp), near))

    def forcing_step(way, comp, arrived):
        return add(local_forcing(way, comp), mul(get(coef_c, way, comp), arrived))

    def send_forcing_edges(stage, way):
        send_edges(stage, way, [local_forcing(way, comp) for comp in range(comps)])

    sublane = lax.broadcasted_iota(jnp.int32, (comps, rows, lanes), 1)
    lane = lax.broadcasted_iota(jnp.int32, (comps, rows, lanes), 2)
    plane = lax.broadcasted_iota(jnp.int32, (rows, lanes), 0)

    def turned_back(vectors):
        return [
            turn[0][j] * vectors[0] + turn[1][j] * vectors[1] + turn[2][j] * vectors[2]
            for j in range(comps)
        ]

    def without_halo():
        for z in range(depth):
            for part in range(2):
                here = cur[z, part]
                up = jnp.where(sublane == 0, 0.0, pltpu.roll(here, 1, 1))
                down = jnp.where(sublane == rows - 1, 0.0, pltpu.roll(here, rows - 1, 1))
                left = jnp.where(lane == 0, 0.0, pltpu.roll(here, 1, 2))
                right = jnp.where(lane == lanes - 1, 0.0, pltpu.roll(here, lanes - 1, 2))
                driven = src[z, part] + COUPLING * ((down + up) + (right + left))
                for comp, value in enumerate(turned_back(driven)):
                    rhs[z, comp, part] = value
            forward(z, [get(rhs, z, comp) for comp in range(comps)])
        backward()

    def with_halo(above, below):
        for z in range(depth):
            added = []
            for part in range(2):
                outer = jnp.where(
                    sublane == 0,
                    halo_in[above, 0, z, part],
                    jnp.where(sublane == rows - 1, halo_in[below, 1, z, part], 0.0),
                )
                added.append(turned_back(COUPLING * outer))
            forward(z, [
                add(get(rhs, z, comp), (added[0][comp], added[1][comp])) for comp in range(comps)
            ])
        backward()

    def forward(z, forcings):
        for comp, forcing in enumerate(forcings):
            if z:
                forcing = add(forcing, mul(get(piv, z - 1, comp), get(sol, z - 1, comp)))
            put(sol, forcing, z, comp)

    def backward():
        for comp in range(comps):
            value = mul(get(piv, last, comp), get(sol, last, comp))
            put(sol, value, last, comp)
            for z in range(last - 1, -1, -1):
                value = mul(get(piv, z, comp), add(get(sol, z, comp), value))
                put(sol, value, z, comp)

    near_way = lax.div(k * 2, nk)
    far_way = 1 - near_way

    @pl.when(place_of(near_way) == 0)
    def _():
        relay_coefficients(near_way)

    loads[3].wait()
    loads[5].wait()
    turn = rotation(angles)
    ender = place_of(far_way) == nk - 1

    def combine_whole(stage):
        for way in range(2):
            for comp in range(comps):
                total = get(whole_in, stage, way, nk - 2, comp)
                for far in range(nk - 2, 0, -1):
                    passed = mul(get(whole_in, 0, way, far - 1, comp), total)
                    total = add(get(whole_in, stage, way, far - 1, comp), passed)
                put(chain_in, total, stage, way, comp)

    def with_mate_halo(number):
        for side in range(2):
            @pl.when(crossing(side))
            def _():
                wait_slot(number, SWEEPS, side)

        with_halo(slot_of(number, 0), slot_of(number, 1))

    def far_first():
        relay_coefficients(far_way)
        relay(1, far_way, forcing_step)

    early = paired & jnp.logical_not(ender)
    for number in range(SWEEPS):
        stage = number + 1
        without_halo()
        if number == 0:
            @pl.when(place_of(near_way) > 0)
            def _():
                relay_coefficients(near_way)

            relay(stage, near_way, forcing_step)

            @pl.when(early)
            def _():
                far_first()
        else:
            @pl.when(direct)
            def _():
                for way in range(2):
                    send_whole(stage, way, [local_forcing(way, comp) for comp in range(comps)])

            @pl.when(jnp.logical_not(direct))
            def _():
                relay(stage, near_way, forcing_step)

        wait_halo(number)
        with_halo(number, number)
        send_forcing_edges(stage, near_way)
        if number == 0:
            @pl.when(paired & ender)
            def _():
                mate_columns()

            @pl.when(jnp.logical_not(early))
            def _():
                far_first()

            send_forcing_edges(stage, far_way)

            @pl.when(direct)
            def _():
                for way in range(2):
                    send_whole(0, way, [get(coef_c, way, comp) for comp in range(comps)])

            @pl.when(paired & jnp.logical_not(ender))
            def _():
                mate_columns()

            wait_edges(0)
        else:
            send_forcing_edges(stage, far_way)

            @pl.when(paired & ender)
            def _():
                with_mate_halo(number)

            @pl.when(direct)
            def _():
                wait_whole(0)
                wait_whole(stage)
                combine_whole(stage)

            @pl.when(jnp.logical_not(direct))
            def _():
                relay(stage, far_way, forcing_step)

            @pl.when(paired & jnp.logical_not(ender))
            def _():
                with_mate_halo(number)

        wait_edges(stage)
        if stage == SWEEPS:
            @pl.when(paired)
            def _():
                wait_edges(SWEEPS + 1)
                for side in range(2):
                    @pl.when(crossing(side))
                    def _():
                        add_from_mates(stage, side)

        first_in, last_in = [], []
        for comp in range(comps):
            arrived, leaving = [], []
            for way in range(2):
                total = None
                for far in range(nk - 1, 0, -1):
                    term = get(edge_in, stage, way, far - 1, comp)
                    if total is not None:
                        term = add(term, mul(get(edge_in, 0, way, far - 1, comp), total))
                    total = term
                inner = get(chain_in, stage, way, comp)
                value = tuple(
                    jnp.where(
                        plane == 0,
                        total[part][:1],
                        jnp.where(plane == rows - 1, total[part][1:], inner[part]),
                    )
                    for part in range(2)
                )
                arrived.append(value)
                leaving.append(forcing_step(way, comp, value))
            p_in, q_in = get(chain_in, 0, 0, comp), get(chain_in, 0, 1, comp)
            p_out, q_out = get(chain_out, 0, 0, comp), get(chain_out, 0, 1, comp)
            above = add(arrived[0], mul(p_in, leaving[1]))
            below = add(arrived[1], mul(q_in, leaving[0]))
            first_in.append(mul(above, inverse(one_less(mul(q_out, p_in)))))
            last_in.append(mul(below, inverse(one_less(mul(p_out, q_in)))))
        for chunk in range(CHUNKS):
            for z in range(chunk * per, (chunk + 1) * per):
                solved = []
                for comp in range(comps):
                    value = add(
                        mul(get(vec_v, z, comp), first_in[comp]),
                        mul(get(vec_u, z, comp), last_in[comp]),
                    )
                    solved.append(add(get(sol, z, comp), value))
                    if stage == SWEEPS - 1:
                        put(sol, solved[comp], z, comp)
                for part in range(2):
                    for c in range(comps):
                        value = (
                            turn[c][0] * solved[0][part]
                            + turn[c][1] * solved[1][part]
                            + turn[c][2] * solved[2][part]
                        )
                        if stage == SWEEPS:
                            out[z, part, c] = value
                        else:
                            cur[z, part, c] = value
                            halo_out[stage, 0, z, part, c] = value[:1]
                            halo_out[stage, 1, z, part, c] = value[rows - 1:]
            if stage < SWEEPS:
                send_halo(stage, chunk)
        if stage == SWEEPS - 1:
            for side in range(2):
                @pl.when(crossing(side))
                def _():
                    send_to_mates(side)

    for number in range(SWEEPS):
        finish_halo(number)
    for stage in range(SWEEPS + 1):
        finish_edges(stage)
    for stage in range(SWEEPS):
        finish_chain(stage)

    @pl.when(direct)
    def _():
        finish_whole()

    @pl.when(jnp.logical_not(direct))
    def _():
        finish_chain(SWEEPS)

    @pl.when(paired)
    def _():
        finish_edges(SWEEPS + 1)
        diag_copy().wait_send()
        for way in range(2):
            for far in range(1, nk):
                @pl.when(place_of(way) < nk - far)
                def _():
                    mate_copy(way, far).wait_send()


def local(ni, nk, field, source, classes, boundary, conductance, angles, strengths):
    depth, _, comps, rows, lanes = field.shape
    block = (depth, 2, comps, rows, lanes)
    lines = (depth, comps, 2, rows, lanes)
    ends = (2, comps, 2, rows, lanes)
    row_lines = (depth, comps, 2, 1, lanes)
    vmem = lambda *shape: pltpu.VMEM(shape, jnp.float32)
    dma = lambda *shape: pltpu.SemaphoreType.DMA(shape)
    whole = pl.BlockSpec(memory_space=pltpu.HBM)
    return pl.pallas_call(
        functools.partial(kernel, ni, nk),
        out_shape=pltpu.VMEM(block, jnp.float32),
        in_specs=[whole] * 7,
        out_specs=pl.BlockSpec(memory_space=pltpu.VMEM),
        scratch_shapes=[
            *[pltpu.SMEM(v.shape, jnp.float32) for v in (conductance, angles, strengths)],
            vmem(*block), vmem(*block),
            pltpu.VMEM(classes.shape, jnp.int32), pltpu.VMEM(boundary.shape, jnp.int32),
            vmem(*lines), vmem(*lines), vmem(*lines), vmem(*lines), vmem(*lines),
            vmem(*ends), vmem(*ends), vmem(*ends),
            vmem(SWEEPS, 2, depth, 2, comps, 1, lanes), vmem(SWEEPS + 1, 2, depth, 2, comps, 1, lanes),
            vmem(SWEEPS + 1, *ends), vmem(SWEEPS + 1, *ends),
            vmem(SWEEPS + 2, 2, comps, 2, 2, lanes), vmem(SWEEPS + 2, 2, nk - 1, comps, 2, 2, lanes),
            vmem(SWEEPS + 1, *ends), vmem(SWEEPS + 1, 2, nk - 1, *ends[1:]),
            vmem(depth, 2, rows, lanes), vmem(depth, 2, 1, lanes), vmem(depth, 2, 1, lanes),
            vmem(*row_lines), vmem(*row_lines), vmem(*row_lines),
            vmem(comps, 2, 2, 1, lanes), vmem(2, nk - 1, comps, 2, 2, 1, lanes),
            dma(7), dma(SWEEPS, 2, CHUNKS), dma(SWEEPS + 1, 2, CHUNKS),
            dma(SWEEPS + 1, 2, comps), dma(SWEEPS + 1, 2, comps),
            dma(SWEEPS + 2, 2, nk - 1), dma(SWEEPS + 2, 2, nk - 1),
            pltpu.SemaphoreType.DMA, pltpu.SemaphoreType.DMA, dma(2, nk - 1), dma(2, nk - 1),
            dma(SWEEPS + 1, 2, nk - 1), dma(SWEEPS + 1, 2, nk - 1),
        ],
        compiler_params=pltpu.CompilerParams(
            collective_id=0, has_side_effects=True, vmem_limit_bytes=56 * 1024 * 1024
        ),
    )(field, source, classes, boundary, conductance, angles, strengths)


def solution(mesh):
    in_specs = (
        P("gz", None, None, "xy", None),
        P("gz", None, None, "xy", None),
        P("gz", "xy", None),
        P("gz", "xy", None),
        P(),
        P(),
        P(),
    )
    out_specs = P("gz", None, None, "xy", None)
    body = functools.partial(local, mesh.shape["xy"], mesh.shape["gz"])
    return jax.shard_map(body, mesh=mesh, in_specs=in_specs, out_specs=out_specs, check_vma=False)
```
